256 devices in a mesh: seq: 32 (over z_hi, y, core), wgt: 8 (over x, z_lo).
Axes of the slice: x: 4, y: 4, z: 8 (z_hi: 4, z_lo: 2; z = z_hi * 2 + z_lo), core: 2. Of those that a mesh axis runs over, the one named last changes fastest.
Arguments:
- hidden: bfloat16 [12288, 5376], P('seq', 'wgt'), may hold values from -6 to 6
- q_weight: bfloat16 [2, 5376, 2048], P(None, 'seq', 'wgt'), may hold values from -448 to 448, as said below
- k_weight: bfloat16 [2, 5376, 1024], P(None, 'seq', 'wgt'), may hold values from -448 to 448, as said below
- v_weight: bfloat16 [2, 5376, 1024], P(None, 'seq', 'wgt'), may hold values from -448 to 448, as said below
- o_weight: bfloat16 [2, 2048, 5376], P(None, 'seq', 'wgt'), may hold values from -448 to 448, as said below
- q_scale: int32 [2, 42, 16], P(None, None, 'wgt'), may hold values from 113 to 117
- k_scale: int32 [2, 42, 8], P(None, None, 'wgt'), may hold values from 113 to 117
- v_scale: int32 [2, 42, 8], P(None, None, 'wgt'), may hold values from 113 to 117
- o_scale: int32 [2, 16, 42], replicated, may hold values from 113 to 117
- in_gain: float32 [2, 5376], replicated, may hold values from 0.5 to 1.5
- post_gain: float32 [2, 5376], P(None, 'wgt'), may hold values from 0.5 to 1.5
- q_gain: float32 [2, 128], replicated, may hold values from 0.1 to 1.9
- k_gain: float32 [2, 128], replicated, may hold values from 0.1 to 1.9
- windows: int32 [2], replicated, may hold values from 512 to 1024, as said below
Outputs:
- state: bfloat16 [12288, 5376], P('seq', 'wgt')
The draws below stay inside these ranges and needn't reach their ends.
Inputs may be any that keep to these rules, and one draw needn't show every extreme that they name: `q_weight`: every entry is a finite value of the e4m3 floating-point format: sign, 3 mantissa bits, exponents of that format. `k_weight`: every entry is a finite value of the e4m3 floating-point format. `v_weight`: every entry is a finite value of the e4m3 floating-point format. `o_weight`: every entry is a finite value of the e4m3 floating-point format. `windows`: one layer's window is exactly 1024.
All inputs are finite; a program needn't handle non-finite values.
Results may differ from the reference program's by a relative error of at most 0.0095.
Values may be sent and summed in bfloat16 or wider, within the bound.
A program may use at most 128 MiB of HBM per device.

```python
import jax
import jax.numpy as jnp
from jax import lax

D = 5376
HEADS = 16
KV_HEADS = 8
HD = 128
BLOCK = 128
WINDOW = 1024
LAYERS = 2
TOK_DEV = 384
TOKENS = 12288
HALO = 3


def e4m3_values(key, shape):
    sign_key, expo_key, mant_key = jax.random.split(key, 3)
    sign = jax.random.randint(sign_key, shape, 0, 2)
    expo = jax.random.randint(expo_key, shape, 4, 15)
    mant = jax.random.randint(mant_key, shape, 0, 8)
    value = (1.0 - 2.0 * sign.astype(jnp.float32)) * (1.0 + mant.astype(jnp.float32) / 8.0) * jnp.exp2(expo.astype(jnp.float32) - 7.0)
    return value.astype(jnp.bfloat16)


def draw_q_weight(key, part):
    return e4m3_values(jax.random.fold_in(key, 11), (LAYERS, D, HEADS * HD))


def draw_k_weight(key, part):
    return e4m3_values(jax.random.fold_in(key, 12), (LAYERS, D, KV_HEADS * HD))


def draw_v_weight(key, part):
    return e4m3_values(jax.random.fold_in(key, 13), (LAYERS, D, KV_HEADS * HD))


def draw_o_weight(key, part):
    return e4m3_values(jax.random.fold_in(key, 14), (LAYERS, HEADS * HD, D))


def draw_windows(key, part):
    length_key = jax.random.fold_in(key, 21)
    pick_key = jax.random.fold_in(key, 22)
    lengths = jax.random.randint(length_key, (LAYERS,), WINDOW // 2, WINDOW + 1)
    chosen = jax.random.randint(pick_key, (), 0, LAYERS)
    layer_ids = jnp.arange(LAYERS, dtype=jnp.int32)
    return jnp.where(layer_ids == chosen, WINDOW, lengths).astype(jnp.int32)


def set_ends(array, own_key, smallest, largest):
    longest = array.shape.index(max(array.shape))
    spots = []
    for shift in (0, 1):
        where = [jax.random.randint(jax.random.fold_in(own_key, axis), (), 0, length) for axis, length in enumerate(array.shape)]
        where[longest] = (where[longest] + shift) % array.shape[longest]
        spots.append(tuple(where))
    return array.at[spots[0]].set(smallest).at[spots[1]].set(largest)


def level_of(stream_key, shape, shards, low, top_value):
    loudness = 1.0
    for axis_at, shards_of in shards:
        steps = jax.random.uniform(jax.random.fold_in(jax.random.fold_in(stream_key, 6), axis_at), (shards_of,), jnp.float32, low / len(shards), top_value / len(shards))
        loudness = loudness * jnp.repeat(jnp.exp(steps), shape[axis_at] // shards_of).reshape((-1,) + (1,) * (len(shape) - 1 - axis_at))
    return loudness


def noise(own_key, shape, spread, most, pieces=(), kind=jnp.bfloat16):
    drawn = spread * jax.random.normal(own_key, shape, jnp.float32)
    if pieces:
        drawn = drawn * level_of(own_key, shape, pieces, -0.22, 0.18)
    return jnp.clip(drawn, -most, most).astype(kind)


def setup_inputs(seed: int = 0) -> dict:
    key_list = jax.random.split(jax.random.key(seed), 15)
    hidden = noise(key_list[0], (TOKENS, D), 1.0, 6.0, ((0, 32), (1, 8)))
    q_weight = draw_q_weight(jax.random.fold_in(key_list[14], 71), 0)
    k_weight = draw_k_weight(jax.random.fold_in(key_list[14], 71), 0)
    v_weight = draw_v_weight(jax.random.fold_in(key_list[14], 71), 0)
    o_weight = draw_o_weight(jax.random.fold_in(key_list[14], 71), 0)
    q_scale = set_ends(jax.random.randint(key_list[5], (LAYERS, D // BLOCK, HEADS * HD // BLOCK), 113, 118), jax.random.fold_in(key_list[5], 1), 113, 117).astype(jnp.int32)
    k_scale = set_ends(jax.random.randint(key_list[6], (LAYERS, D // BLOCK, KV_HEADS * HD // BLOCK), 113, 118), jax.random.fold_in(key_list[6], 1), 113, 117).astype(jnp.int32)
    v_scale = set_ends(jax.random.randint(key_list[7], (LAYERS, D // BLOCK, KV_HEADS * HD // BLOCK), 113, 118), jax.random.fold_in(key_list[7], 1), 113, 117).astype(jnp.int32)
    o_scale = set_ends(jax.random.randint(key_list[8], (LAYERS, HEADS * HD // BLOCK, D // BLOCK), 113, 118), jax.random.fold_in(key_list[8], 1), 113, 117).astype(jnp.int32)
    in_gain = jnp.clip(1.0 + 0.1 * jax.random.normal(key_list[9], (LAYERS, D), jnp.float32), 0.5, 1.5)
    post_gain = jnp.clip(1.0 + 0.1 * jax.random.normal(key_list[10], (LAYERS, D), jnp.float32), 0.5, 1.5)
    q_gain = jnp.clip(1.0 + 0.18 * jax.random.normal(key_list[11], (LAYERS, HD), jnp.float32), 0.1, 1.9)
    k_gain = jnp.clip(1.0 + 0.18 * jax.random.normal(key_list[12], (LAYERS, HD), jnp.float32), 0.1, 1.9)
    windows = draw_windows(jax.random.fold_in(key_list[14], 71), 0)
    return dict(hidden=hidden, q_weight=q_weight, k_weight=k_weight, v_weight=v_weight, o_weight=o_weight, q_scale=q_scale, k_scale=k_scale, v_scale=v_scale, o_scale=o_scale, in_gain=in_gain, post_gain=post_gain, q_gain=q_gain, k_gain=k_gain, windows=windows)


eps = 1e-06
query_scale = 168.0 ** (-0.5)
rope_base = 10000.0

def rmsnorm(values, gain):
    return values * lax.rsqrt(lax.optimization_barrier(jnp.mean(values * values, axis=-1, keepdims=True)) + eps) * gain.astype(jnp.float32)

def rotate(values, position):
    half = values.shape[-1] // 2
    inverse = rope_base ** (-jnp.arange(half, dtype=jnp.float32) * 2.0 / values.shape[-1])
    angles = position.astype(jnp.float32)[:, None] * inverse[None, :]
    cosine = jnp.cos(angles)[:, None, :]
    sine = jnp.sin(angles)[:, None, :]
    first = values[..., :half]
    second = values[..., half:]
    return jnp.concatenate([first * cosine - second * sine, second * cosine + first * sine], axis=-1)

def dequantize(codes, scale_codes):
    factor = jnp.exp2(scale_codes.astype(jnp.float32) - 127.0)
    factor = jnp.repeat(jnp.repeat(factor, BLOCK, axis=0), BLOCK, axis=1)
    return (codes.astype(jnp.float32) * factor).astype(jnp.bfloat16)

def attend(queries, key_rows, value_rows, window):
    span = TOK_DEV
    reach = HALO * TOK_DEV
    groups = HEADS // KV_HEADS
    key_padded = jnp.pad(key_rows, ((reach, 0), (0, 0), (0, 0)))
    value_padded = jnp.pad(value_rows, ((reach, 0), (0, 0), (0, 0)))

    def one_block(index):
        begin = (index * span).astype(jnp.int32)
        query_block = lax.dynamic_slice_in_dim(queries, begin, span, 0).reshape(span, KV_HEADS, groups, HD).astype(jnp.float32)
        key_block = lax.dynamic_slice_in_dim(key_padded, begin, reach + span, 0).astype(jnp.float32)
        value_block = lax.dynamic_slice_in_dim(value_padded, begin, reach + span, 0).astype(jnp.float32)
        scores = jnp.einsum('qkgd,skd->kgqs', query_block, key_block)
        query_pos = begin + jnp.arange(span, dtype=jnp.int32)
        key_pos = begin - reach + jnp.arange(reach + span, dtype=jnp.int32)
        gap = query_pos[:, None] - key_pos[None, :]
        allowed = (key_pos[None, :] >= 0) & (gap >= 0) & (gap < window)
        scores = jnp.where(allowed, scores, -1e+30)
        top = lax.optimization_barrier(jnp.max(scores, axis=-1, keepdims=True))
        expval = jnp.exp(scores - top)
        weights = (expval / lax.optimization_barrier(jnp.sum(expval, axis=-1, keepdims=True))).astype(jnp.bfloat16)
        mixed = jnp.einsum('kgqs,skd->qkgd', weights.astype(jnp.float32), value_block)
        return mixed.reshape(span, HEADS * HD).astype(jnp.bfloat16)
    blocks = lax.map(one_block, jnp.arange(TOKENS // TOK_DEV, dtype=jnp.int32))
    return blocks.reshape(TOKENS, HEADS * HD)

def reference(hidden, q_weight, k_weight, v_weight, o_weight, q_scale, k_scale, v_scale, o_scale, in_gain, post_gain, q_gain, k_gain, windows):
    position = jnp.arange(TOKENS, dtype=jnp.int32)
    state = hidden
    for layer_idx in range(LAYERS):
        normed = rmsnorm(state.astype(jnp.float32), in_gain[layer_idx]).astype(jnp.bfloat16)
        queries = jnp.dot(normed, dequantize(q_weight[layer_idx], q_scale[layer_idx]), preferred_element_type=jnp.float32)
        key_rows = jnp.dot(normed, dequantize(k_weight[layer_idx], k_scale[layer_idx]), preferred_element_type=jnp.float32)
        value_rows = jnp.dot(normed, dequantize(v_weight[layer_idx], v_scale[layer_idx]), preferred_element_type=jnp.float32)
        queries = (rotate(rmsnorm(queries.reshape(TOKENS, HEADS, HD), q_gain[layer_idx]), position) * query_scale).astype(jnp.bfloat16)
        key_rows = rotate(rmsnorm(key_rows.reshape(TOKENS, KV_HEADS, HD), k_gain[layer_idx]), position).astype(jnp.bfloat16)
        value_rows = value_rows.reshape(TOKENS, KV_HEADS, HD).astype(jnp.bfloat16)
        mixed = attend(queries, key_rows, value_rows, windows[layer_idx])
        projected = jnp.dot(mixed, dequantize(o_weight[layer_idx], o_scale[layer_idx]), preferred_element_type=jnp.float32)
        state = (state.astype(jnp.float32) + rmsnorm(projected, post_gain[layer_idx])).astype(jnp.bfloat16)
    return state
```

```python
import jax
import jax.numpy as jnp
from jax import lax
from jax.experimental import pallas as pl
from jax.experimental.pallas import tpu as pltpu
from jax.sharding import PartitionSpec as P

HD = 128
BLOCK = 128
LAYERS = 2
NSEQ = 32
NWGT = 8
TOK = 384
WIDTH = 672
ROWS = 168
D = 5376
MESH = pl.DeviceIdType.MESH

eps = 1e-06
query_scale = 168.0 ** (-0.5)
rope_base = 10000.0
BF = jnp.bfloat16
F32 = jnp.float32


def contract_rows(a, b):
    return lax.dot_general(a, b, (((0,), (0,)), ((), ())), preferred_element_type=F32)


def kernel(
    hid, wa, wb, wo, gin, gpost, qg, kg, cosine, sine, windows,
    out,
    H, WA, WB, O, MX, KV, SS, acc, Q, SC, PB, proj,
    w_recv, o_recv, h_recv, mx_recv, kv_recv, sib_recv, ss_recv, send,
):
    s = lax.axis_index("seq")
    w = lax.axis_index("wgt")
    core = s % 2
    y = (s // 2) % 4
    zh = s // 8
    x = w // 2
    zl = w % 2

    def seq_of(dz, dy):
        return ((zh + dz) % 4) * 8 + ((y + dy) % 4) * 2 + core

    def wgt_of(dx, dz):
        return ((x + dx) % 4) * 2 + (zl + dz) % 2

    sibling = s + 1 - 2 * core

    def on_seq(i):
        return {"seq": i, "wgt": w}

    def on_wgt(i):
        return {"seq": s, "wgt": i}

    def copy(src, dst, send_sem, recv_sem, device):
        return pltpu.make_async_remote_copy(
            src_ref=src,
            dst_ref=dst,
            send_sem=send_sem,
            recv_sem=recv_sem,
            device_id=device,
            device_id_type=MESH,
        )

    here = on_seq(sibling)

    def arrived(dst, sem):
        copy(dst, dst, send.at[0, 0], sem, here).wait_recv()

    def sent(region, sem):
        copy(region, region, sem, w_recv.at[0, 0, 0, 0], here).wait_send()

    def w_slot(l, half, index):
        if half == 0:
            return WA.at[l, index]
        if half == 1:
            return WB.at[l, index]
        return O.at[l, 2 * index + (half - 2)]

    def w_sem(l, half, dz, dy):
        if half < 2:
            return w_recv.at[l, half, dz, dy]
        return o_recv.at[l, half - 2, dz, dy]

    def w_to(l, half, owner, rel, step):
        slot = w_slot(l, half, owner)
        to = ((rel[0] - step[0]) % 4, (rel[1] - step[1]) % 4)
        copy(
            slot, slot, send.at[l, half], w_sem(l, half, *to), on_seq(seq_of(*step))
        ).start()

    def w_to_sibling(l, half, owner):
        slot = w_slot(l, half, owner)
        copy(slot, slot, send.at[l, half], sib_recv.at[l, half], here).start()

    def w_own(l, halves):
        for half in halves:
            for step in ((0, 1), (0, 3), (1, 0), (3, 0)):
                w_to(l, half, s, (0, 0), step)
            w_to_sibling(l, half, s)

    def w_event(l, half, dz, dy):
        owner = seq_of(dz, dy)
        arrived(w_slot(l, half, owner), w_sem(l, half, dz, dy))
        first = half % 2 == 0
        if dy == 0:
            w_to(l, half, owner, (dz, 0), (0, 1))
            w_to(l, half, owner, (dz, 0), (0, 3))
            if dz == 3 and first:
                w_to(l, half, owner, (3, 0), (1, 0))
            if dz == 1 and not first:
                w_to(l, half, owner, (1, 0), (3, 0))
        elif dy == 3 and first:
            w_to(l, half, owner, (dz, 3), (0, 1))
        elif dy == 1 and not first:
            w_to(l, half, owner, (dz, 1), (0, 3))
        w_to_sibling(l, half, owner)

    def h_to(l, piece, rel, step):
        slot = H.at[l, 4 * wgt_of(*rel) + piece]
        to = ((rel[0] - step[0]) % 4, (rel[1] - step[1]) % 2)
        copy(
            slot, slot, send.at[l, 4], h_recv.at[l, to[0], to[1], piece], on_wgt(wgt_of(*step))
        ).start()

    def h_wait(l, piece, dx, dz):
        arrived(H.at[l, 4 * wgt_of(dx, dz) + piece], h_recv.at[l, dx, dz, piece])

    def h_event(l, piece, dx, dz):
        h_wait(l, piece, dx, dz)
        if (dx, dz) == (0, 1):
            h_to(l, piece, (0, 1), (1, 0))
            h_to(l, piece, (0, 1), (3, 0))
        elif dx == 3 and piece < 2:
            h_to(l, piece, (3, dz), (1, 0))
        elif dx == 1 and piece >= 2:
            h_to(l, piece, (1, dz), (3, 0))

    def m_to(l, head, rel, step):
        slot = MX.at[l, wgt_of(*rel), head]
        to = ((rel[0] - step[0]) % 4, (rel[1] - step[1]) % 2)
        copy(
            slot, slot, send.at[l, 5], mx_recv.at[l, to[0], to[1], head], on_wgt(wgt_of(*step))
        ).start()

    def m_event(l, head, dx, dz):
        arrived(MX.at[l, wgt_of(dx, dz), head], mx_recv.at[l, dx, dz, head])
        if (dx, dz) == (0, 1):
            m_to(l, head, (0, 1), (1, 0))
            m_to(l, head, (0, 1), (3, 0))
        elif dx == 3 and head == 0:
            m_to(l, head, (3, dz), (1, 0))
        elif dx == 1 and head == 1:
            m_to(l, head, (1, dz), (3, 0))

    peers = [(dx, dz) for dz in range(2) for dx in range(4) if (dx, dz) != (0, 0)]

    def share_squares(l, kind, row):
        SS[l, kind, w] = jnp.broadcast_to(row, (8, TOK))
        slot = SS.at[l, kind, w]
        for rel in peers:
            copy(
                slot, slot, send.at[l, 6 + kind], ss_recv.at[l, kind], on_wgt(wgt_of(*rel))
            ).start()

    def all_squares(l, kind):
        arrived(SS.at[l, kind, pl.ds(0, 7)], ss_recv.at[l, kind])
        return jnp.sum(SS[l, kind], axis=0)[0:1]

    for l in range(LAYERS):
        WA[l, s] = wa[l]
        WB[l, s] = wb[l]
        for half in range(2):
            O[l, 2 * s + half] = wo[l, half]
    out[...] = hid[...]

    barrier = pltpu.get_barrier_semaphore()
    neighbours = [here]
    neighbours += [on_seq(seq_of(*step)) for step in ((0, 1), (0, 3), (1, 0), (3, 0))]
    neighbours += [on_wgt(wgt_of(*rel)) for rel in peers]
    after = on_seq((s + 2) % NSEQ)
    neighbours += [after, on_seq((s + NSEQ - 2) % NSEQ)]
    neighbours += [on_seq((s + NSEQ - 3 + 6 * core) % NSEQ)]
    for device in neighbours:
        pl.semaphore_signal(barrier, inc=1, device_id=device, device_id_type=MESH)
    pl.semaphore_wait(barrier, len(neighbours))

    w_own(0, (0, 1))

    def layer(l, carry):
        squares = jnp.zeros((1, TOK), F32)
        for i in range(4):
            state = out[i].astype(F32)
            H[l, 4 * w + i] = (state * gin[l, i]).astype(BF)
            squares += jnp.sum(state * state, axis=0, keepdims=True)
        for i in range(4):
            h_to(l, (0, 3, 1, 2)[i], (0, 0), (0, 1))
            h_to(l, i, (0, 0), (1, 0))
            h_to(l, 3 - i, (0, 0), (3, 0))
        share_squares(l, 0, squares)
        acc[...] = jnp.zeros_like(acc)

        timed = []
        for i in range(4):
            timed.append((3 * (i + 1), h_event, i, 3, 0))
            timed.append((3 * (i + 1), h_event, 3 - i, 1, 0))
            timed.append((5 * (i + 1), h_event, (0, 3, 1, 2)[i], 0, 1))
        for t, i in ((14, 0), (14, 3), (19.5, 1), (19.5, 2)):
            timed.append((t, h_event, i, 2, 0))
        for t, i in ((17, 0), (22.5, 3)):
            timed.append((t, h_event, i, 3, 1))
            timed.append((t, h_event, i, 1, 1))

        def w_times(t_own, t_z, t_opp, t_diag, t_z2, t_last, half0):
            events = []
            for k in range(2):
                half = half0 + k
                events += [(t_own[k], w_event, half, 0, 3), (t_own[k], w_event, half, 0, 1)]
                events += [(t_z[k], w_event, half, 3, 0), (t_z[k], w_event, half, 1, 0)]
                events += [(t_opp, w_event, half, 0, 2)]
                for dz in (3, 1):
                    events += [(t_diag[k], w_event, half, dz, 3), (t_diag[k], w_event, half, dz, 1)]
                    events += [(t_last[0], w_event, half, dz, 2)]
                events += [(t_z2, w_event, half, 2, 0)]
                events += [(t_last[1], w_event, half, 2, 3), (t_last[1], w_event, half, 2, 1)]
                events += [(t_last[2], w_event, half, 2, 2)]
            return events

        timed += w_times((2, 4), (4.5, 9), 6.2, (9.5, 13), 14.5, (16.5, 19, 22), 0)
        timed.sort(key=lambda e: e[0])
        for _, event, *which in timed:
            event(l, *which)
        w_own(l, (2, 3))
        for half, buf in ((0, WA), (1, WB)):
            arrived(buf.at[l, pl.ds(0, 16)], sib_recv.at[l, half])

        def multiply(t, carry):
            group = t // 4
            k = group % 4
            index = 4 * wgt_of(k * (k + 1) // 2, group // 4) + t % 4
            piece = H[l, index]
            acc[0:256] += contract_rows(WA[l, index], piece)
            acc[256:512] += contract_rows(WB[l, index], piece)
            return carry

        def while_arriving(j, carry):
            lax.fori_loop(10 * j, 10 * j + 10, multiply, 0)
            for dx in (3, 1):
                h_wait(l, 1 + j, dx, 1)

            @pl.when(j == 0)
            def _():
                h_to(l, 1, (3, 1), (1, 0))

            @pl.when(j == 1)
            def _():
                h_to(l, 2, (1, 1), (3, 0))

            return carry

        lax.fori_loop(0, 2, while_arriving, 0)
        o_events = w_times((1, 1), (2, 2), 3, (4, 4), 5, (6, 7, 8), 2)
        o_events.sort(key=lambda e: e[0])
        for t, event, *which in o_events:
            if t <= 2:
                event(l, *which)
        lax.fori_loop(20, 28, multiply, 0)

        def last_pieces(j, carry):
            high = j // 2
            odd = j % 2
            piece = (1 - high) * 3 * odd + high * (1 + odd)
            h_wait(l, piece, 2, 1)
            return multiply(28 + piece, carry)

        lax.fori_loop(0, 4, last_pieces, 0)

        row = lax.rsqrt(all_squares(l, 0) / D + eps)

        def head_of(rows, gain):
            values = acc[rows] * row
            values *= lax.rsqrt(jnp.mean(values * values, axis=0, keepdims=True) + eps)
            values *= gain[l]
            first = values[0:64]
            second = values[64:128]
            c = cosine[...]
            n = sine[...]
            return first * c - second * n, second * c + first * n

        first, second = head_of(pl.ds(256, 128), kg)
        KV[l, 3, 0:64] = first.astype(BF)
        KV[l, 3, 64:128] = second.astype(BF)
        KV[l, 3, 128:256] = (acc[384:512] * row).astype(BF)

        def kv_full(slot):
            copy(
                KV.at[l, slot], KV.at[l, 1], send.at[l, 8], kv_recv.at[l, 1], after
            ).start()

        def kv_sibling(slot):
            copy(
                KV.at[l, slot], KV.at[l, 2], send.at[l, 9], kv_recv.at[l, 2], here
            ).start()

        late = pl.ds(128, 256)

        def kv_far(slot, device):
            copy(
                KV.at[l, slot, :, late],
                KV.at[l, 0, :, late],
                send.at[l, 10],
                kv_recv.at[l, 0],
                device,
            ).start()

        kv_full(3)

        @pl.when(core == 0)
        def _():
            kv_sibling(3)

        @pl.when(core == 1)
        def _():
            kv_far(3, on_seq((s + 3) % NSEQ))

        for h in range(2):
            first, second = head_of(pl.ds(128 * h, 128), qg)
            Q[h, 0:64] = (first * query_scale).astype(BF)
            Q[h, 64:128] = (second * query_scale).astype(BF)

        arrived(KV.at[l, 1], kv_recv.at[l, 1])

        @pl.when(core == 0)
        def _():
            kv_far(1, here)

        @pl.when(core == 1)
        def _():
            kv_sibling(1)

        for t, event, *which in o_events:
            if 2 < t <= 5:
                event(l, *which)
        arrived(KV.at[l, 2], kv_recv.at[l, 2])
        arrived(KV.at[l, 0, :, late], kv_recv.at[l, 0])

        window = windows[l]

        def attend(h, carry):
            SC[128:384] = contract_rows(KV[l, 0, 0:128, 128:384], Q[h])
            for j in range(1, 4):
                SC[384 * j : 384 * (j + 1)] = contract_rows(KV[l, j, 0:128], Q[h])

            def soften(c, carry):
                lanes = pl.ds(pl.multiple_of(128 * c, 128), 128)
                keys = lax.broadcasted_iota(jnp.int32, (1408, 128), 0) + 128
                gap = lax.broadcasted_iota(jnp.int32, (1408, 128), 1) + 128 * c + 1152 - keys
                allowed = (gap >= 0) & (gap < window) & (keys >= 1152 - TOK * s)
                scores = jnp.where(allowed, SC[128:1536, lanes], -1e30)
                scores = jnp.exp(scores - jnp.max(scores, axis=0, keepdims=True))
                total = jnp.sum(scores, axis=0, keepdims=True)
                PB[128:1536, lanes] = (scores * (1.0 / total)).astype(BF)
                return carry

            lax.fori_loop(0, 3, soften, 0)
            mixed = jnp.dot(
                KV[l, 0, 128:256, 128:384], PB[128:384], preferred_element_type=F32
            )
            for j in range(1, 4):
                mixed += jnp.dot(
                    KV[l, j, 128:256], PB[384 * j : 384 * (j + 1)], preferred_element_type=F32
                )
            MX[l, w, h] = mixed.astype(BF)
            for step in ((0, 1), (1, 0), (3, 0)):
                m_to(l, h, (0, 0), step)
            return carry

        lax.fori_loop(0, 2, attend, 0)

        for t, event, *which in o_events:
            if t > 5:
                event(l, *which)
        for head in range(2):
            m_event(l, head, 3, 0)
            m_event(l, head, 1, 0)
            m_event(l, head, 0, 1)
        for head in range(2):
            m_event(l, head, 2, 0)
        for head in range(2):
            m_event(l, head, 3, 1)
            m_event(l, head, 1, 1)
        arrived(O.at[l, pl.ds(0, 16)], sib_recv.at[l, 2])
        arrived(O.at[l, pl.ds(0, 16)], sib_recv.at[l, 3])
        proj[...] = jnp.zeros_like(proj)

        def project(t, carry):
            k = t % 4
            index = wgt_of(k * (k + 1) // 2, t // 4)
            block = O[l, pl.ds(8 * index, 8)].reshape(256, WIDTH)
            proj[...] += contract_rows(block, MX[l, index].reshape(256, TOK))
            return carry

        lax.fori_loop(0, 7, project, 0)
        m_event(l, 0, 2, 1)
        m_event(l, 1, 2, 1)
        lax.fori_loop(7, 8, project, 0)

        squares = jnp.zeros((1, TOK), F32)
        for i in range(4):
            part = proj[ROWS * i : ROWS * (i + 1)]
            squares += jnp.sum(part * part, axis=0, keepdims=True)
        share_squares(l, 1, squares)

        @pl.when(l == 0)
        def _():
            w_own(1, (0, 1))

        row = lax.rsqrt(all_squares(l, 1) / D + eps)
        for i in range(4):
            post = proj[ROWS * i : ROWS * (i + 1)] * row * gpost[l, i]
            out[i] = (out[i].astype(F32) + post).astype(BF)

        sent(WA.at[l, pl.ds(0, 31)], send.at[l, 0])
        sent(WB.at[l, pl.ds(0, 31)], send.at[l, 1])
        sent(O.at[l, pl.ds(0, 31)], send.at[l, 2])
        sent(O.at[l, pl.ds(0, 31)], send.at[l, 3])
        sent(H.at[l, pl.ds(0, 28)], send.at[l, 4])
        sent(MX.at[l, pl.ds(0, 7)], send.at[l, 5])
        for kind in range(2):
            sent(SS.at[l, kind, pl.ds(0, 7)], send.at[l, 6 + kind])
        sent(KV.at[l, 1], send.at[l, 8])
        sent(KV.at[l, 2], send.at[l, 9])
        sent(KV.at[l, 0, :, late], send.at[l, 10])
        return carry

    lax.fori_loop(0, LAYERS, layer, 0)


def row_factors(scale_codes, first_row, rows):
    blocks = (first_row + jnp.arange(rows, dtype=jnp.int32)) // BLOCK
    pick = blocks[:, None] == jnp.arange(scale_codes.shape[1], dtype=jnp.int32)[None, :]
    factor = jnp.exp2(scale_codes.astype(F32) - 127.0)
    return jnp.sum(jnp.where(pick[None, :, :, None], factor[:, None], 0.0), axis=2)


def per_device(
    hidden,
    q_weight,
    k_weight,
    v_weight,
    o_weight,
    q_scale,
    k_scale,
    v_scale,
    o_scale,
    in_gain,
    post_gain,
    q_gain,
    k_gain,
    windows,
):
    s = lax.axis_index("seq")
    w = lax.axis_index("wgt")
    scales = jnp.concatenate([q_scale, k_scale, v_scale], axis=2)
    factors = jnp.repeat(row_factors(scales, ROWS * s, ROWS), BLOCK, axis=2).astype(BF)
    wa = q_weight * factors[:, :, :256]
    wb = jnp.concatenate([k_weight, v_weight], axis=2) * factors[:, :, 256:]
    o_rows = jnp.exp2(
        lax.dynamic_slice_in_dim(o_scale, s // 2, 1, axis=1).astype(F32) - 127.0
    )
    columns = (w * WIDTH + jnp.arange(WIDTH, dtype=jnp.int32)) // BLOCK
    pick = columns[:, None] == jnp.arange(D // BLOCK, dtype=jnp.int32)[None, :]
    o_factor = jnp.sum(jnp.where(pick[None], o_rows, 0.0), axis=2).astype(BF)
    wo = (o_weight * o_factor[:, None, :]).reshape(LAYERS, 2, 32, WIDTH)
    gin = lax.dynamic_slice_in_dim(in_gain, w * WIDTH, WIDTH, axis=1)
    gin = gin.reshape(LAYERS, 4, ROWS, 1)
    gpost = post_gain.reshape(LAYERS, 4, ROWS, 1)
    half = HD // 2
    position = s * TOK + jnp.arange(TOK, dtype=jnp.int32)
    inverse = rope_base ** (-jnp.arange(half, dtype=F32) * 2.0 / HD)
    angles = inverse[:, None] * position.astype(F32)[None, :]
    hid = hidden.T.reshape(4, ROWS, TOK)

    vmem = pl.BlockSpec(memory_space=pltpu.VMEM)
    dma = pltpu.SemaphoreType.DMA
    state = pl.pallas_call(
        kernel,
        out_shape=jax.ShapeDtypeStruct((4, ROWS, TOK), BF),
        in_specs=[vmem] * 10 + [pl.BlockSpec(memory_space=pltpu.SMEM)],
        out_specs=vmem,
        scratch_shapes=[
            pltpu.VMEM((LAYERS, 32, ROWS, TOK), BF),
            pltpu.VMEM((LAYERS, NSEQ, ROWS, 256), BF),
            pltpu.VMEM((LAYERS, NSEQ, ROWS, 256), BF),
            pltpu.VMEM((LAYERS, 2 * NSEQ, 32, WIDTH), BF),
            pltpu.VMEM((LAYERS, NWGT, 2, HD, TOK), BF),
            pltpu.VMEM((LAYERS, 4, 2 * HD, TOK), BF),
            pltpu.VMEM((LAYERS, 2, NWGT, 8, TOK), F32),
            pltpu.VMEM((512, TOK), F32),
            pltpu.VMEM((2, HD, TOK), BF),
            pltpu.VMEM((4 * TOK, TOK), F32),
            pltpu.VMEM((4 * TOK, TOK), BF),
            pltpu.VMEM((WIDTH, TOK), F32),
            dma((LAYERS, 2, 4, 4)),
            dma((LAYERS, 2, 4, 4)),
            dma((LAYERS, 4, 2, 4)),
            dma((LAYERS, 4, 2, 2)),
            dma((LAYERS, 3)),
            dma((LAYERS, 4)),
            dma((LAYERS, 2)),
            dma((LAYERS, 11)),
        ],
        compiler_params=pltpu.CompilerParams(
            collective_id=0, has_side_effects=True, vmem_limit_bytes=60 * 1024 * 1024
        ),
    )(
        hid,
        wa,
        wb,
        wo,
        gin,
        gpost,
        q_gain.reshape(LAYERS, HD, 1),
        k_gain.reshape(LAYERS, HD, 1),
        jnp.cos(angles),
        jnp.sin(angles),
        windows,
    )
    return state.reshape(WIDTH, TOK).T


def solution(mesh):
    in_specs = (
        P("seq", "wgt"),
        P(None, "seq", "wgt"),
        P(None, "seq", "wgt"),
        P(None, "seq", "wgt"),
        P(None, "seq", "wgt"),
        P(None, None, "wgt"),
        P(None, None, "wgt"),
        P(None, None, "wgt"),
        P(),
        P(),
        P(None, "wgt"),
        P(),
        P(),
        P(),
    )
    return jax.shard_map(
        per_device, mesh=mesh, in_specs=in_specs, out_specs=P("seq", "wgt"), check_vma=False
    )
```

```python
import jax
import jax.numpy as jnp
from jax import lax
from jax.experimental import pallas as pl
from jax.experimental.pallas import tpu as pltpu
from jax.sharding import PartitionSpec as P

HD = 128
BLOCK = 128
LAYERS = 2
NSEQ = 32
NWGT = 8
TOK = 384
WIDTH = 672
ROWS = 168
D = 5376
MESH = pl.DeviceIdType.MESH

eps = 1e-06
query_scale = 168.0 ** (-0.5)
rope_base = 10000.0
H_BY_Z = ((1, 2), (0, 1, 2, 3))
BF = jnp.bfloat16
F32 = jnp.float32


def contract_rows(a, b):
    return lax.dot_general(a, b, (((0,), (0,)), ((), ())), preferred_element_type=F32)


FIRST_HOPS = 8.2


def w_schedule(half0):
    events = []
    for k in range(2):
        half = half0 + k
        if half0 == 0:
            own, zs, opp, last = (2.5, 4.3)[k], (4.4, 8.2)[k], 6.2, ((19, 20.8)[k], 22.7)
            diag, edge, z2 = ((8.3, 9.7), (11.6, 13.4))[k], (15.5, 17.2), 11.6
        else:
            own, zs, opp, last = 1, 2, 3, (6, 7)
            diag, edge, z2 = (4, 4), (6, 6), 5
        events += [(own, half, 0, 3), (own, half, 0, 1), (opp, half, 0, 2)]
        for i, dz in enumerate((3, 1)):
            events += [(zs, half, dz, 0), (diag[i], half, dz, 3), (diag[i], half, dz, 1)]
            events += [(edge[i], half, dz, 2)]
        events += [(z2, half, 2, 0), (last[0], half, 2, 3), (last[0], half, 2, 1)]
        events += [(last[1], half, 2, 2)]
    return sorted(events, key=lambda e: e[0])


def kernel(
    hid, wa, wb, wo, gains, cosine, sine, windows,
    out,
    H, WA, WB, O, MX, KV, SS, acc, Q, KX, SC, PB, TOT, MIX, RB, proj,
    w_recv, o_recv, h_recv, mx_recv, kv_recv, sib_recv, ss_recv, send,
):
    s = lax.axis_index("seq")
    w = lax.axis_index("wgt")
    core = s % 2
    y = (s // 2) % 4
    zh = s // 8
    x = w // 2
    zl = w % 2

    def seq_of(dz, dy):
        return ((zh + dz) % 4) * 8 + ((y + dy) % 4) * 2 + core

    def wgt_of(dx, dz):
        return ((x + dx) % 4) * 2 + (zl + dz) % 2

    sibling = s + 1 - 2 * core

    def on_seq(i):
        return {"seq": i, "wgt": w}

    def on_wgt(i):
        return {"seq": s, "wgt": i}

    def copy(src, dst, send_sem, recv_sem, device):
        return pltpu.make_async_remote_copy(
            src_ref=src,
            dst_ref=dst,
            send_sem=send_sem,
            recv_sem=recv_sem,
            device_id=device,
            device_id_type=MESH,
        )

    here = on_seq(sibling)

    def arrived(dst, sem):
        copy(dst, dst, send.at[0, 0], sem, here).wait_recv()

    def sent(region, sem):
        copy(region, region, sem, w_recv.at[0, 0, 0, 0], here).wait_send()

    def w_slot(l, half, index):
        if half == 0:
            return WA.at[l, index]
        if half == 1:
            return WB.at[l, index]
        return O.at[l, 2 * index + (half - 2)]

    def w_sem(l, half, dz, dy):
        if half < 2:
            return w_recv.at[l, half, dz, dy]
        return o_recv.at[l, half - 2, dz, dy]

    def w_to(l, half, owner, rel, step):
        slot = w_slot(l, half, owner)
        to = ((rel[0] - step[0]) % 4, (rel[1] - step[1]) % 4)
        copy(
            slot, slot, send.at[l, half], w_sem(l, half, *to), on_seq(seq_of(*step))
        ).start()

    def w_to_sibling(l, half, owner):
        slot = w_slot(l, half, owner)
        copy(slot, slot, send.at[l, half], sib_recv.at[l, half], here).start()

    def w_own(l, halves):
        for half in halves:
            for step in ((0, 1), (0, 3), (1, 0), (3, 0)):
                w_to(l, half, s, (0, 0), step)
            w_to_sibling(l, half, s)

    def w_event(l, half, dz, dy):
        owner = seq_of(dz, dy)
        arrived(w_slot(l, half, owner), w_sem(l, half, dz, dy))
        first = half % 2 == 0
        if dy == 0:
            if dz == 3 and first:
                w_to(l, half, owner, (3, 0), (1, 0))
            if dz == 1 and not first:
                w_to(l, half, owner, (1, 0), (3, 0))
            w_to(l, half, owner, (dz, 0), (0, 1))
            w_to(l, half, owner, (dz, 0), (0, 3))
        elif dy == 3 and first:
            w_to(l, half, owner, (dz, 3), (0, 1))
        elif dy == 1 and not first:
            w_to(l, half, owner, (dz, 1), (0, 3))
        w_to_sibling(l, half, owner)

    def h_to(l, piece, rel, step):
        slot = H.at[l, 4 * wgt_of(*rel) + piece]
        to = ((rel[0] - step[0]) % 4, (rel[1] - step[1]) % 2)
        copy(
            slot, slot, send.at[l, 4], h_recv.at[l, to[0], to[1], piece], on_wgt(wgt_of(*step))
        ).start()

    def h_event(l, piece, dx, dz):
        arrived(H.at[l, 4 * wgt_of(dx, dz) + piece], h_recv.at[l, dx, dz, piece])
        if (dx, dz) == (0, 1):
            h_to(l, piece, (0, 1), (1, 0))
            h_to(l, piece, (0, 1), (3, 0))
        elif (dx, dz) == (2, 0):
            if piece in H_BY_Z[l]:
                h_to(l, piece, (2, 0), (0, 1))
        elif dz == 1 and piece in H_BY_Z[l]:
            pass
        elif dx == 3 and piece < 2:
            h_to(l, piece, (3, dz), (1, 0))
        elif dx == 1 and piece >= 2:
            h_to(l, piece, (1, dz), (3, 0))

    def m_to(l, head, rel, step):
        slot = MX.at[l, wgt_of(*rel), head]
        to = ((rel[0] - step[0]) % 4, (rel[1] - step[1]) % 2)
        copy(
            slot, slot, send.at[l, 5], mx_recv.at[l, to[0], to[1], head], on_wgt(wgt_of(*step))
        ).start()

    def m_event(l, head, dx, dz):
        arrived(MX.at[l, wgt_of(dx, dz), head], mx_recv.at[l, dx, dz, head])
        if (dx, dz) == (0, 1):
            m_to(l, head, (0, 1), (1, 0))
            m_to(l, head, (0, 1), (3, 0))
        elif (dx, dz) == (2, 0):
            m_to(l, head, (2, 0), (0, 1))
        elif (dx, dz, head) == (3, 0, 0):
            m_to(l, head, (3, 0), (1, 0))
        elif (dx, dz, head) == (1, 0, 1):
            m_to(l, head, (1, 0), (3, 0))

    peers = [(dx, dz) for dz in range(2) for dx in range(4) if (dx, dz) != (0, 0)]

    def share_squares(l, kind, row):
        SS[l, kind, w] = row
        slot = SS.at[l, kind, w]
        for rel in peers:
            copy(
                slot, slot, send.at[l, 6 + kind], ss_recv.at[l, kind], on_wgt(wgt_of(*rel))
            ).start()

    def all_squares(l, kind):
        arrived(SS.at[l, kind, pl.ds(0, 7)], ss_recv.at[l, kind])
        return jnp.sum(SS[l, kind], axis=0)

    def gain(l, kind, rows):
        return gains[rows, 2 * kind + l : 2 * kind + l + 1]

    for l in range(LAYERS):
        WA[l, s] = wa[l]
        WB[l, s] = wb[l]
        for half in range(2):
            O[l, 2 * s + half] = wo[l, half]
        for slot in range(3):
            KV[l, slot] = jnp.zeros((2, HD, TOK), BF)
    out[...] = hid[...]

    barrier = pltpu.get_barrier_semaphore()
    neighbours = [here]
    neighbours += [on_seq(seq_of(*step)) for step in ((0, 1), (0, 3), (1, 0), (3, 0))]
    neighbours += [on_wgt(wgt_of(*rel)) for rel in peers]
    after = on_seq((s + 2) % NSEQ)
    neighbours += [after, on_seq((s + NSEQ - 2) % NSEQ)]
    neighbours += [on_seq((s + NSEQ - 3 + 6 * core) % NSEQ)]
    for device in neighbours:
        pl.semaphore_signal(barrier, inc=1, device_id=device, device_id_type=MESH)
    pl.semaphore_wait(barrier, len(neighbours))

    w_own(0, (0, 1))

    def layer(l):
        squares = jnp.zeros((1, TOK), F32)
        for i in range(4):
            state = out[i].astype(F32)
            H[l, 4 * w + i] = (state * gain(l, 0, pl.ds(ROWS * i, ROWS))).astype(BF)
            squares += jnp.sum(state * state, axis=0, keepdims=True)
        for i in range(4):
            h_to(l, i, (0, 0), (1, 0))
            h_to(l, 3 - i, (0, 0), (3, 0))
        share_squares(l, 0, squares)
        acc[...] = jnp.zeros_like(acc)

        def multiply(group, carry):
            k = group % 4
            first = 4 * wgt_of(k * (k + 1) // 2, group // 4)
            for buf, rows in ((WA, pl.ds(0, 256)), (WB, pl.ds(256, 256))):
                total = acc[rows]
                for i in range(4):
                    total += contract_rows(buf[l, first + i], H[l, first + i])
                acc[rows] = total
            return carry

        def weights_here():
            for half, buf in ((0, WA), (1, WB)):
                arrived(buf.at[l, pl.ds(0, 16)], sib_recv.at[l, half])

        timed = []

        def at(t, step, *args):
            timed.append((t, step, args))

        if l == 0:
            for t, *which in w_schedule(0):
                at(t, w_event, l, *which)
            at(24.4, weights_here)
        else:
            for t, *which in w_schedule(0):
                if t > FIRST_HOPS:
                    at(max(t - 7.5, 1), w_event, l, *which)
            at(17.1, weights_here)
            for t, *which in w_schedule(2):
                at((0, 17.15, 18, 19, 20.6, 21.5, 26.1, 28.6)[t], w_event, l, *which)

        def h_own_by_z():
            for i in (0, 3, 1, 2):
                h_to(l, i, (0, 0), (0, 1))

        if l == 0:
            pair = (14.2, 17, 19.7, 22.5)
            far = (14.2, 14.2, 17, 17)
            late_x = (19.9, 22.5, 25.4, 28.1)
            late_z = (29.5, 29.5, 29.5, 29.5)
            at(8.25, h_own_by_z)
            at(21, w_own, l, (2, 3))
            blocks = ((24.5, 0, 3), (25.5, 3, 5), (28.2, 5, 7), (29.6, 7, 8))
        else:
            pair = (3.2, 6, 8.8, 11.5)
            far = (14.5, 14.5, 20, 20)
            late_x = (17.2, 22.8, 25.6, 28.4)
            late_z = (20.5, 20.5, 25.7, 25.7)
            at(0, h_own_by_z)
            at(11.5, w_own, l, (2, 3))
            blocks = ((17.2, 0, 3), (20.4, 3, 5), (26, 7, 8), (28.5, 5, 7))
        for i in range(4):
            near = (3.2, 6, 8.8, 11.5)[i]
            piece = (0, 3, 1, 2)[i]
            at(near, h_event, l, i, 3, 0)
            at(near, h_event, l, 3 - i, 1, 0)
            at(pair[i], h_event, l, piece, 0, 1)
            at(far[i], h_event, l, piece, 2, 0)
            at(late_x[i], h_event, l, piece, 3, 1)
            at(late_x[i], h_event, l, piece, 1, 1)
            at(late_z[i], h_event, l, piece, 2, 1)

        def multiply_groups(first, last):
            lax.fori_loop(first, last, multiply, 0)

        for t, first, last in blocks:
            at(t, multiply_groups, first, last)
        timed.sort(key=lambda e: e[0])
        for _, step, args in timed:
            step(*args)

        def o_event(*stages):
            if l == 0:
                for t, *which in w_schedule(2):
                    if t in stages:
                        w_event(l, *which)

        o_event(1)
        row = lax.rsqrt(all_squares(l, 0) / D + eps)

        def head_of(rows, kind):
            values = acc[rows] * row
            values *= lax.rsqrt(jnp.mean(values * values, axis=0, keepdims=True) + eps)
            values *= gain(l, kind, pl.ds(WIDTH, HD))
            first = values[0:64]
            second = values[64:128]
            c = cosine[...]
            n = sine[...]
            return first * c - second * n, second * c + first * n

        late = pl.ds(128, 256)

        def kv_full(part):
            copy(
                KV.at[l, 3, part], KV.at[l, 1, part],
                send.at[l, 8], kv_recv.at[l, 1, part], after,
            ).start()

        def kv_sibling(slot, part):
            copy(
                KV.at[l, slot, part], KV.at[l, 2, part],
                send.at[l, 9], kv_recv.at[l, 2, part], here,
            ).start()

        def kv_far(slot, part, device):
            copy(
                KV.at[l, slot, part, :, late], KV.at[l, 0, part, :, late],
                send.at[l, 10], kv_recv.at[l, 0, part], device,
            ).start()

        def kv_own(part):
            direct = s < NSEQ - 2
            if part == 1:
                direct &= y != 3

                @pl.when((y == 3) & (s < NSEQ - 2))
                def _():
                    for half in range(2):
                        rows = pl.ds(64 * half, 64)
                        copy(
                            KV.at[l, 3, 1, rows], RB.at[l, rows],
                            send.at[l, 8], kv_recv.at[l, 3, half], on_seq(s - 6),
                        ).start()

            @pl.when(direct)
            def _():
                kv_full(part)

            @pl.when(core == 0)
            def _():
                kv_sibling(3, part)

        first, second = head_of(pl.ds(256, 128), 1)
        KV[l, 3, 0, 0:64] = first.astype(BF)
        KV[l, 3, 0, 64:128] = second.astype(BF)
        kv_own(0)
        KV[l, 3, 1] = (acc[384:512] * row).astype(BF)
        kv_own(1)

        for h in range(2):
            first, second = head_of(pl.ds(128 * h, 128), 0)
            Q[h, 0:64] = (first * query_scale).astype(BF)
            Q[h, 64:128] = (second * query_scale).astype(BF)

        window = windows[l]

        def attend(slot):
            skip = 128 if slot == 0 else 0
            rows = TOK - skip
            KX[0:rows] = KV[l, slot, 0, :, skip:TOK].T

            def one_head(h, carry):
                SC[0:rows] = jnp.dot(KX[0:rows], Q[h], preferred_element_type=F32)
                keys = lax.broadcasted_iota(jnp.int32, (rows, 128), 0) + (TOK * slot + skip)
                for c in range(3):
                    lanes = pl.ds(128 * c, 128)
                    gap = lax.broadcasted_iota(jnp.int32, (rows, 128), 1) + (
                        128 * c + 3 * TOK
                    ) - keys
                    allowed = (gap < window) & (keys >= 3 * TOK - TOK * s)
                    if slot == 3:
                        allowed &= gap >= 0
                    weight = jnp.where(allowed, jnp.exp(SC[0:rows, lanes]), 0.0)
                    total = jnp.sum(weight, axis=0, keepdims=True)
                    if slot != 3:
                        total += TOT[h, :, lanes]
                    TOT[h, :, lanes] = total
                    PB[0:rows, lanes] = weight.astype(BF)
                mixed = jnp.dot(
                    KV[l, slot, 1, :, skip:TOK], PB[0:rows], preferred_element_type=F32
                )
                if slot != 3:
                    mixed += MIX[h]
                MIX[h] = mixed
                return carry

            lax.fori_loop(0, 2, one_head, 0)

        o_event(2, 3)
        attend(3)

        @pl.when((core == 1) & (s < NSEQ - 3))
        def _():
            for part in range(2):
                kv_far(3, part, on_seq((s + 3) % NSEQ))

        @pl.when((y == 0) & (s < NSEQ - 8))
        def _():
            for half in range(2):
                rows = pl.ds(64 * half, 64)
                arrived(RB.at[l, rows], kv_recv.at[l, 3, half])
                copy(
                    RB.at[l, rows], KV.at[l, 1, 1, rows],
                    send.at[l, 11], kv_recv.at[l, 1, 1], on_seq(s + 8),
                ).start()

        o_event(4, 5)
        for part in range(2):

            @pl.when(s >= 2)
            def _():
                arrived(KV.at[l, 1, part], kv_recv.at[l, 1, part])

            @pl.when((core == 0) & (s >= 2))
            def _():
                kv_far(1, part, here)

            @pl.when((core == 1) & (s >= 2))
            def _():
                kv_sibling(1, part)

        attend(1)

        @pl.when(s >= 1)
        def _():
            for part in range(2):
                arrived(KV.at[l, 2, part], kv_recv.at[l, 2, part])

        attend(2)

        @pl.when(s >= 3)
        def _():
            for part in range(2):
                arrived(KV.at[l, 0, part, :, late], kv_recv.at[l, 0, part])

        attend(0)
        for h in range(2):
            MX[l, w, h] = (MIX[h] * (1.0 / TOT[h])).astype(BF)
            for step in ((0, 1), (1, 0), (3, 0)):
                m_to(l, h, (0, 0), step)

        proj[...] = jnp.zeros_like(proj)

        def project(group, carry):
            k = group % 4
            index = wgt_of(k * (k + 1) // 2, group // 4)
            block = O[l, pl.ds(8 * index, 8)].reshape(256, WIDTH)
            proj[...] += contract_rows(block, MX[l, index].reshape(256, TOK))
            return carry

        m_event(l, 0, 3, 0)
        m_event(l, 1, 1, 0)
        m_event(l, 0, 0, 1)
        o_event(6)
        m_event(l, 1, 3, 0)
        m_event(l, 0, 1, 0)
        m_event(l, 1, 0, 1)
        if l == 0:
            w_own(1, (0, 1))
        m_event(l, 0, 2, 0)
        m_event(l, 1, 2, 0)
        o_event(7)
        arrived(O.at[l, pl.ds(0, 16)], sib_recv.at[l, 2])
        arrived(O.at[l, pl.ds(0, 16)], sib_recv.at[l, 3])
        lax.fori_loop(0, 5, project, 0)
        for head in range(2):
            m_event(l, head, 3, 1)
            m_event(l, head, 1, 1)
        lax.fori_loop(5, 7, project, 0)
        m_event(l, 0, 2, 1)
        m_event(l, 1, 2, 1)
        lax.fori_loop(7, 8, project, 0)

        squares = jnp.zeros((1, TOK), F32)
        for i in range(4):
            part = proj[ROWS * i : ROWS * (i + 1)]
            squares += jnp.sum(part * part, axis=0, keepdims=True)
        share_squares(l, 1, squares)

        if l == 0:
            for t, *which in w_schedule(0):
                if t <= FIRST_HOPS:
                    w_event(1, *which)
        row = lax.rsqrt(all_squares(l, 1) / D + eps)
        for i in range(4):
            post = proj[ROWS * i : ROWS * (i + 1)] * row * gain(l, 1, pl.ds(ROWS * i, ROWS))
            out[i] = (out[i].astype(F32) + post).astype(BF)

        sent(WA.at[l, pl.ds(0, 31)], send.at[l, 0])
        sent(WB.at[l, pl.ds(0, 31)], send.at[l, 1])
        sent(O.at[l, pl.ds(0, 31)], send.at[l, 2])
        sent(O.at[l, pl.ds(0, 31)], send.at[l, 3])
        sent(H.at[l, pl.ds(0, 28)], send.at[l, 4])
        sent(MX.at[l, pl.ds(0, 7)], send.at[l, 5])
        for kind in range(2):
            sent(SS.at[l, kind, pl.ds(0, 7)], send.at[l, 6 + kind])

        @pl.when(s < NSEQ - 2)
        def _():
            sent(KV.at[l, 1], send.at[l, 8])

        @pl.when((y == 0) & (s < NSEQ - 8))
        def _():
            sent(RB.at[l], send.at[l, 11])

        @pl.when((core == 0) | (s >= 2))
        def _():
            sent(KV.at[l, 2], send.at[l, 9])

        @pl.when(((core == 0) & (s >= 2)) | ((core == 1) & (s < NSEQ - 3)))
        def _():
            sent(KV.at[l, 0, :, :, late], send.at[l, 10])


    for l in range(LAYERS):
        layer(l)


def row_factors(scale_codes, first_row, rows):
    blocks = (first_row + jnp.arange(rows, dtype=jnp.int32)) // BLOCK
    pick = blocks[:, None] == jnp.arange(scale_codes.shape[1], dtype=jnp.int32)[None, :]
    factor = jnp.exp2(scale_codes.astype(F32) - 127.0)
    return jnp.sum(jnp.where(pick[None, :, :, None], factor[:, None], 0.0), axis=2)


def per_device(
    hidden,
    q_weight,
    k_weight,
    v_weight,
    o_weight,
    q_scale,
    k_scale,
    v_scale,
    o_scale,
    in_gain,
    post_gain,
    q_gain,
    k_gain,
    windows,
):
    s = lax.axis_index("seq")
    w = lax.axis_index("wgt")
    scales = jnp.concatenate([q_scale, k_scale, v_scale], axis=2)
    factors = jnp.repeat(row_factors(scales, ROWS * s, ROWS), BLOCK, axis=2).astype(BF)
    wa = q_weight * factors[:, :, :256]
    wb = jnp.concatenate([k_weight, v_weight], axis=2) * factors[:, :, 256:]
    o_rows = jnp.exp2(
        lax.dynamic_slice_in_dim(o_scale, s // 2, 1, axis=1).astype(F32) - 127.0
    )
    columns = (w * WIDTH + jnp.arange(WIDTH, dtype=jnp.int32)) // BLOCK
    pick = columns[:, None] == jnp.arange(D // BLOCK, dtype=jnp.int32)[None, :]
    o_factor = jnp.sum(jnp.where(pick[None], o_rows, 0.0), axis=2).astype(BF)
    wo = (o_weight * o_factor[:, None, :]).reshape(LAYERS, 2, 32, WIDTH)
    gin = lax.dynamic_slice_in_dim(in_gain, w * WIDTH, WIDTH, axis=1)
    gains = jnp.concatenate(
        [
            jnp.concatenate([gin, post_gain, jnp.zeros((4, WIDTH), F32)], axis=0),
            jnp.concatenate([q_gain, k_gain, jnp.zeros((4, HD), F32)], axis=0),
        ],
        axis=1,
    ).T
    half = HD // 2
    position = s * TOK + jnp.arange(TOK, dtype=jnp.int32)
    inverse = rope_base ** (-jnp.arange(half, dtype=F32) * 2.0 / HD)
    angles = inverse[:, None] * position.astype(F32)[None, :]
    hid = hidden.T.reshape(4, ROWS, TOK)

    vmem = pl.BlockSpec(memory_space=pltpu.VMEM)
    dma = pltpu.SemaphoreType.DMA
    state = pl.pallas_call(
        kernel,
        out_shape=jax.ShapeDtypeStruct((4, ROWS, TOK), BF),
        in_specs=[vmem] * 7 + [pl.BlockSpec(memory_space=pltpu.SMEM)],
        out_specs=vmem,
        scratch_shapes=[
            pltpu.VMEM((LAYERS, 32, ROWS, TOK), BF),
            pltpu.VMEM((LAYERS, NSEQ, ROWS, 256), BF),
            pltpu.VMEM((LAYERS, NSEQ, ROWS, 256), BF),
            pltpu.VMEM((LAYERS, 2 * NSEQ, 32, WIDTH), BF),
            pltpu.VMEM((LAYERS, NWGT, 2, HD, TOK), BF),
            pltpu.VMEM((LAYERS, 4, 2, HD, TOK), BF),
            pltpu.VMEM((LAYERS, 2, NWGT, 1, TOK), F32),
            pltpu.VMEM((512, TOK), F32),
            pltpu.VMEM((2, HD, TOK), BF),
            pltpu.VMEM((TOK, HD), BF),
            pltpu.VMEM((TOK, TOK), F32),
            pltpu.VMEM((TOK, TOK), BF),
            pltpu.VMEM((2, 1, TOK), F32),
            pltpu.VMEM((2, HD, TOK), F32),
            pltpu.VMEM((LAYERS, HD, TOK), BF),
            pltpu.VMEM((WIDTH, TOK), F32),
            dma((LAYERS, 2, 4, 4)),
            dma((LAYERS, 2, 4, 4)),
            dma((LAYERS, 4, 2, 4)),
            dma((LAYERS, 4, 2, 2)),
            dma((LAYERS, 4, 2)),
            dma((LAYERS, 4)),
            dma((LAYERS, 2)),
            dma((LAYERS, 12)),
        ],
        compiler_params=pltpu.CompilerParams(
            collective_id=0, has_side_effects=True, vmem_limit_bytes=44 * 1024 * 1024
        ),
    )(
        hid,
        wa,
        wb,
        wo,
        gains,
        jnp.cos(angles),
        jnp.sin(angles),
        windows,
    )
    return state.reshape(WIDTH, TOK).T


def solution(mesh):
    in_specs = (
        P("seq", "wgt"),
        P(None, "seq", "wgt"),
        P(None, "seq", "wgt"),
        P(None, "seq", "wgt"),
        P(None, "seq", "wgt"),
        P(None, None, "wgt"),
        P(None, None, "wgt"),
        P(None, None, "wgt"),
        P(),
        P(),
        P(None, "wgt"),
        P(),
        P(),
        P(),
    )
    return jax.shard_map(
        per_device, mesh=mesh, in_specs=in_specs, out_specs=P("seq", "wgt"), check_vma=False
    )
```

```python
import jax
import jax.numpy as jnp
from jax import lax
from jax.experimental import pallas as pl
from jax.experimental.pallas import tpu as pltpu
from jax.sharding import PartitionSpec as P

HD = 128
BLOCK = 128
LAYERS = 2
NSEQ = 32
NWGT = 8
TOK = 384
WIDTH = 672
ROWS = 168
D = 5376
MESH = pl.DeviceIdType.MESH

eps = 1e-06
query_scale = 168.0 ** (-0.5)
rope_base = 10000.0
BF = jnp.bfloat16
F32 = jnp.float32


def contract_rows(a, b):
    return lax.dot_general(a, b, (((0,), (0,)), ((), ())), preferred_element_type=F32)


Y_US = {"w": 1.9, "o": 1.08, "k": 2.15}
Z_US = {"w": 3.8, "o": 2.15}
X_US = {"h": 2.85, "m": 1.1}
ZP_US = {"h": 2.85, "m": 1.1}
LAT = {"y": 2.2, "z": 2.8, "x": 2.2, "p": 2.2}
H_BY_Z = ((1, 2), (0, 1, 2, 3))


def w_forwards(half, dz, dy):
    first = half in (1, 2)
    steps = []
    if dy == 0:
        if dz == 3 and first:
            steps.append((1, 0))
        if dz == 1 and not first:
            steps.append((3, 0))
        steps += [(0, 1), (0, 3)]
    elif dy == 3 and first:
        steps.append((0, 1))
    elif dy == 1 and not first:
        steps.append((0, 3))
    return steps


def a_forwards(by_z, piece, dx, dz):
    if (dx, dz) == (0, 1):
        return [(1, 0), (3, 0)]
    if (dx, dz) == (2, 0):
        return [(0, 1)] if piece in by_z else []
    if dz == 1 and piece in by_z:
        return []
    if dx == 3 and piece < 2:
        return [(1, 0)]
    if dx == 1 and piece >= 2:
        return [(3, 0)]
    return []


M_BY_Z = ((1, 2), (1, 2))
BY_Z = {"h": H_BY_Z, "m": M_BY_Z}


SLACK = ((0.5, 1.0), (4.0, 4.0))


def schedule():
    free = {}
    arrival = {}
    done = {}
    order = []
    now = 0.0

    def link(name, us, lat):
        free[name] = max(free.get(name, 0.0), now) + us
        return free[name] + lat

    def send_w(l, half, rel, step):
        kind = "w" if half < 2 else "o"
        to = ((rel[0] - step[0]) % 4, (rel[1] - step[1]) % 4)
        if step[0]:
            t = link("z" + str(step[0]), Z_US[kind], LAT["z"])
        else:
            t = link("y" + str(step[1]), Y_US[kind], LAT["y"])
        arrival["w", l, half, *to] = t

    def send_a(kind, l, piece, rel, step):
        to = ((rel[0] - step[0]) % 4, (rel[1] - step[1]) % 2)
        if step[0]:
            t = link("x" + str(step[0]), X_US[kind], LAT["x"])
        else:
            t = link("z1", ZP_US[kind], LAT["p"])
        arrival[kind, l, piece, *to] = t

    w_events = lambda l, half0: [("w", l, h, dz, dy) for h in (half0, half0 + 1) for dz in range(4) for dy in range(4) if (dz, dy) != (0, 0)]
    owner = lambda g: ([0, 1, 3, 2][g % 4], g // 4)

    tasks = {}
    for l in range(2):
        tasks["scale", l] = (0.3, [("fin", l - 1)] if l else [], 0)
        tasks["wown", l] = (0.05, [("att0", 0)] if l else [], 1)
        tasks["oown", l] = (0.05, ([("scale", 1)] if l else []) + [("w", l, h, dz, 0) for h in (0, 1) for dz in (1, 2, 3)], 1)
        tasks["hz", l] = (0.05, [("scale", l)] + [("w", l, h, dz, 0) for h in (0, 1) for dz in (1, 3)], 0)
        for half in (0, 1):
            name = ("wsib", l, half)
            tasks[name] = (0.02, [e for e in w_events(l, 0) if e[2] == half] + [("kvsent", 0) if (l, half) == (0, 0) else ("scale", l)], 2 - half)
            for g in range(8):
                ow = owner(g)
                pieces = [("scale", l)] if ow == (0, 0) else [("h", l, i, *ow) for i in range(4)]
                tasks["mm", l, half, g] = (0.45, [name] + pieces, 4 - half)
        tasks["kvsent", l] = (0.15, [("mm", l, 1, g) for g in range(8)], 0)
        tasks["heads", l] = (0.2, [("mm", l, 0, g) for g in range(8)] + [("kvsent", l)], 1)
        tasks["att3", l] = (1.07, [("heads", l)], 3)
        tasks["att1", l] = (1.12, [("att3", l), ("kv1", l)], 3)
        tasks["att2", l] = (1.12, [("att1", l), ("kv2", l)], 3)
        tasks["att0", l] = (1.1, [("att2", l), ("kv0", l)], 0)
        tasks["osib", l] = (0.02, w_events(l, 2) + [("att0", l)], 2)
        for g in range(8):
            ow = owner(g)
            tasks["pj", l, g] = (0.38, [("osib", l), ("att0", l)] + ([] if ow == (0, 0) else [("m", l, i, *ow) for i in range(4)]), 3)
        tasks["share", l] = (0.3, [("pj", l, g) for g in range(8)], 0)
        tasks["fin", l] = (0.3, [("share", l), ("ss", l)], 0)

    def run_task(name):
        nonlocal now
        kind, l = name[0], name[1]
        now += tasks[name][0]
        if kind == "wown":
            for h in (1, 0):
                for step in ((0, 1), (0, 3), (1, 0), (3, 0)):
                    send_w(l, h, (0, 0), step)
        if kind == "oown":
            for h in (2, 3):
                for step in ((0, 1), (0, 3), (1, 0), (3, 0)):
                    send_w(l, h, (0, 0), step)
        if kind == "scale":
            for i in range(4):
                send_a("h", l, i, (0, 0), (1, 0))
                send_a("h", l, 3 - i, (0, 0), (3, 0))
        if kind == "hz":
            for i in (0, 3, 1, 2):
                send_a("h", l, i, (0, 0), (0, 1))
        if kind == "kvsent":
            a = link("y1", Y_US["k"], 2.8)
            b = link("y1", Y_US["k"], 2.8)
            arrival["kv1", l] = b + 0.5
            arrival["kv2", l] = b + 2.3
            arrival["kv0", l] = b + 2.5
        if kind == "att0":
            for i in range(4):
                for piece, step in ((i, (1, 0)), (3 - i, (3, 0)), ((0, 3, 1, 2)[i], (0, 1))):
                    send_a("m", l, piece, (0, 0), step)
        if kind == "share":
            arrival["ss", l] = now + 4.0
        done[name] = now
        order.append(name)

    def run_event(ev):
        nonlocal now
        now += 0.06
        kind = ev[0]
        if kind == "w":
            _, l, half, dz, dy = ev
            for step in w_forwards(half, dz, dy):
                send_w(l, half, (dz, dy), step)
        elif kind in "hm":
            _, l, piece, dx, dz = ev
            for step in a_forwards(BY_Z[kind][l], piece, dx, dz):
                send_a(kind, l, piece, (dx, dz), step)
        done[ev] = now
        order.append(ev)

    def eff(ev):
        t = arrival[ev]
        if ev[0] == "w":
            return t + SLACK[ev[1]][ev[2] // 2]
        if ev[0] in "hm" and ev[3:] == (0, 1):
            return t + 0.5
        return t

    while True:
        pend = [e for e in arrival if e not in done]
        ready = [t for t in tasks if t not in done and all(d in done for d in tasks[t][1])]
        if not pend and not ready:
            break
        urgent = [t for t in ready if tasks[t][2] == 0]
        arrived = [e for e in pend if eff(e) <= now]
        if urgent:
            run_task(min(urgent))
        elif arrived:
            run_event(min(arrived, key=lambda e: (eff(e), e)))
        elif ready:
            run_task(min(ready, key=lambda t: (tasks[t][2], tasks[t][1] and max(done[d] for d in tasks[t][1]) or 0, t)))
        else:
            e = min(pend, key=lambda e: (eff(e), e))
            now = max(now, eff(e))
            run_event(e)
    return order


def kernel(
    hid, wa, wb, wo, gains, cosine, sine, windows,
    out,
    H, WA, WB, O, MX, KV, SS, acc, Q, ROW, KX, SC, PB, TOT, MIX, RB, proj,
    w_recv, o_recv, h_recv, mx_recv, kv_recv, sib_recv, ss_recv, send,
):
    s = lax.axis_index("seq")
    w = lax.axis_index("wgt")
    core = s % 2
    y = (s // 2) % 4
    zh = s // 8
    x = w // 2
    zl = w % 2

    def seq_of(dz, dy):
        return ((zh + dz) % 4) * 8 + ((y + dy) % 4) * 2 + core

    def wgt_of(dx, dz):
        return ((x + dx) % 4) * 2 + (zl + dz) % 2

    sibling = s + 1 - 2 * core

    def on_seq(i):
        return {"seq": i, "wgt": w}

    def on_wgt(i):
        return {"seq": s, "wgt": i}

    def copy(src, dst, send_sem, recv_sem, device):
        return pltpu.make_async_remote_copy(
            src_ref=src,
            dst_ref=dst,
            send_sem=send_sem,
            recv_sem=recv_sem,
            device_id=device,
            device_id_type=MESH,
        )

    here = on_seq(sibling)

    def arrived(dst, sem):
        copy(dst, dst, send.at[0, 0], sem, here).wait_recv()

    def sent(region, sem):
        copy(region, region, sem, w_recv.at[0, 0, 0, 0], here).wait_send()

    def w_slot(l, half, index):
        if half == 0:
            return WA.at[l, index]
        if half == 1:
            return WB.at[l, index]
        return O.at[l, 2 * index + (half - 2)]

    def w_sem(l, half, dz, dy):
        if half < 2:
            return w_recv.at[l, half, dz, dy]
        return o_recv.at[l, half - 2, dz, dy]

    def w_to(l, half, owner, rel, step):
        slot = w_slot(l, half, owner)
        to = ((rel[0] - step[0]) % 4, (rel[1] - step[1]) % 4)
        copy(
            slot, slot, send.at[l, half], w_sem(l, half, *to), on_seq(seq_of(*step))
        ).start()

    def w_to_sibling(l, half, owner):
        slot = w_slot(l, half, owner)
        copy(slot, slot, send.at[l, half], sib_recv.at[l, half], here).start()

    def w_own(l, halves, along="yz"):
        for half in halves:
            if "y" in along:
                w_to(l, half, s, (0, 0), (0, 1))
                w_to(l, half, s, (0, 0), (0, 3))
                w_to_sibling(l, half, s)
            if "z" in along:
                w_to(l, half, s, (0, 0), (1, 0))
                w_to(l, half, s, (0, 0), (3, 0))

    def w_event(l, half, dz, dy):
        owner = seq_of(dz, dy)
        arrived(w_slot(l, half, owner), w_sem(l, half, dz, dy))
        for step in w_forwards(half, dz, dy):
            w_to(l, half, owner, (dz, dy), step)
        w_to_sibling(l, half, owner)

    def h_to(l, piece, rel, step):
        slot = H.at[l, 4 * wgt_of(*rel) + piece]
        to = ((rel[0] - step[0]) % 4, (rel[1] - step[1]) % 2)
        copy(
            slot, slot, send.at[l, 4], h_recv.at[l, to[0], to[1], piece], on_wgt(wgt_of(*step))
        ).start()

    def m_to(l, piece, rel, step):
        slot = MX.at[l, wgt_of(*rel), piece]
        to = ((rel[0] - step[0]) % 4, (rel[1] - step[1]) % 2)
        copy(
            slot, slot, send.at[l, 5], mx_recv.at[l, to[0], to[1], piece], on_wgt(wgt_of(*step))
        ).start()

    def h_event(l, piece, dx, dz):
        arrived(H.at[l, 4 * wgt_of(dx, dz) + piece], h_recv.at[l, dx, dz, piece])
        for step in a_forwards(BY_Z["h"][l], piece, dx, dz):
            h_to(l, piece, (dx, dz), step)

    def m_event(l, piece, dx, dz):
        arrived(MX.at[l, wgt_of(dx, dz), piece], mx_recv.at[l, dx, dz, piece])
        for step in a_forwards(BY_Z["m"][l], piece, dx, dz):
            m_to(l, piece, (dx, dz), step)

    peers = [(dx, dz) for dz in range(2) for dx in range(4) if (dx, dz) != (0, 0)]

    def share_squares(l, kind, row):
        SS[l, kind, w] = row
        slot = SS.at[l, kind, w]
        for rel in peers:
            copy(
                slot, slot, send.at[l, 6 + kind], ss_recv.at[l, kind], on_wgt(wgt_of(*rel))
            ).start()

    def all_squares(l, kind):
        arrived(SS.at[l, kind, pl.ds(0, 7)], ss_recv.at[l, kind])
        return jnp.sum(SS[l, kind], axis=0)

    def gain(l, kind, rows):
        return gains[rows, 2 * kind + l : 2 * kind + l + 1]

    for l in range(LAYERS):
        WA[l, s] = wa[l]
        WB[l, s] = wb[l]
        for half in range(2):
            O[l, 2 * s + half] = wo[l, half]
        for slot in range(3):
            KV[l, slot] = jnp.zeros((2, HD, TOK), BF)
    out[...] = hid[...]

    barrier = pltpu.get_barrier_semaphore()
    neighbours = [here]
    neighbours += [on_seq(seq_of(*step)) for step in ((0, 1), (0, 3), (1, 0), (3, 0))]
    neighbours += [on_wgt(wgt_of(*rel)) for rel in peers]
    after = on_seq((s + 2) % NSEQ)
    neighbours += [after, on_seq((s + NSEQ - 2) % NSEQ)]
    neighbours += [on_seq((s + NSEQ - 3 + 6 * core) % NSEQ)]
    for device in neighbours:
        pl.semaphore_signal(barrier, inc=1, device_id=device, device_id_type=MESH)
    pl.semaphore_wait(barrier, len(neighbours))

    late = pl.ds(128, 256)

    def scale(l):
        squares = jnp.zeros((1, TOK), F32)
        for i in range(4):
            state = out[i].astype(F32)
            H[l, 4 * w + i] = (state * gain(l, 0, pl.ds(ROWS * i, ROWS))).astype(BF)
            squares += jnp.sum(state * state, axis=0, keepdims=True)
        for i in range(4):
            h_to(l, i, (0, 0), (1, 0))
            h_to(l, 3 - i, (0, 0), (3, 0))
        share_squares(l, 0, squares)
        acc[...] = jnp.zeros_like(acc)

    def multiply(l, half, first, last):
        buf, rows = ((WA, pl.ds(0, 256)), (WB, pl.ds(256, 256)))[half]

        def one(group, carry):
            k = group % 4
            index = 4 * wgt_of(k * (k + 1) // 2, group // 4)
            total = acc[rows]
            for i in range(4):
                total += contract_rows(buf[l, index + i], H[l, index + i])
            acc[rows] = total
            return carry

        lax.fori_loop(first, last, one, 0)

    def head_of(l, rows, row, kind):
        values = acc[rows] * row
        values *= lax.rsqrt(jnp.mean(values * values, axis=0, keepdims=True) + eps)
        values *= gain(l, kind, pl.ds(WIDTH, HD))
        first = values[0:64]
        second = values[64:128]
        c = cosine[...]
        n = sine[...]
        return first * c - second * n, second * c + first * n

    def kv_sibling(l, slot, part):
        copy(
            KV.at[l, slot, part], KV.at[l, 2, part],
            send.at[l, 9], kv_recv.at[l, 2, part], here,
        ).start()

    def kv_far(l, slot, part, device):
        copy(
            KV.at[l, slot, part, :, late], KV.at[l, 0, part, :, late],
            send.at[l, 10], kv_recv.at[l, 0, part], device,
        ).start()

    def kv_next(l, part, rows):
        copy(
            KV.at[l, 3, part, rows], KV.at[l, 1, part, rows],
            send.at[l, 8], kv_recv.at[l, 1, part], after,
        ).start()

    corner = [pl.ds(64 + 32 * i, 32) for i in range(2)]

    def keys_values(l):
        row = lax.rsqrt(all_squares(l, 0) / D + eps)
        ROW[...] = row
        KV[l, 3, 1] = (acc[384:512] * row).astype(BF)

        @pl.when((y == 3) & (s < NSEQ - 2))
        def _():
            for i in range(2):
                copy(
                    KV.at[l, 3, 1, corner[i]], RB.at[l, pl.ds(32 * i, 32)],
                    send.at[l, 8], kv_recv.at[l, 3, i], on_seq(s - 6),
                ).start()

        first, second = head_of(l, pl.ds(256, 128), row, 1)
        KV[l, 3, 0, 0:64] = first.astype(BF)
        KV[l, 3, 0, 64:128] = second.astype(BF)

        @pl.when(s < NSEQ - 2)
        def _():
            kv_next(l, 0, pl.ds(0, 128))
            kv_next(l, 1, pl.ds(0, 64))

        @pl.when((y != 3) & (s < NSEQ - 2))
        def _():
            kv_next(l, 1, pl.ds(64, 64))

        @pl.when(core == 0)
        def _():
            for part in range(2):
                kv_sibling(l, 3, part)

        @pl.when((core == 1) & (s < NSEQ - 3))
        def _():
            for part in range(2):
                kv_far(l, 3, part, on_seq((s + 3) % NSEQ))

    def queries(l):
        for h in range(2):
            first, second = head_of(l, pl.ds(128 * h, 128), ROW[...], 0)
            Q[h, 0:64] = (first * query_scale).astype(BF)
            Q[h, 64:128] = (second * query_scale).astype(BF)

    def attend(l, slot):
        skip = 128 if slot == 0 else 0
        rows = TOK - skip
        window = windows[l]
        KX[0:rows] = KV[l, slot, 0, :, skip:TOK].T
        keys = lax.broadcasted_iota(jnp.int32, (rows, 128), 0) + (TOK * slot + skip)
        for h in range(2):
            SC[h, 0:rows] = jnp.dot(KX[0:rows], Q[h], preferred_element_type=F32)
        for h in range(2):
            for c in range(3):
                lanes = pl.ds(128 * c, 128)
                gap = lax.broadcasted_iota(jnp.int32, (rows, 128), 1) + (128 * c + 3 * TOK) - keys
                allowed = (gap < window) & (keys >= 3 * TOK - TOK * s)
                if slot == 3:
                    allowed &= gap >= 0
                weight = jnp.where(allowed, jnp.exp(SC[h, 0:rows, lanes]), 0.0)
                total = jnp.sum(weight, axis=0, keepdims=True)
                if slot != 3:
                    total += TOT[h, :, lanes]
                TOT[h, :, lanes] = total
                PB[h, 0:rows, lanes] = weight.astype(BF)
            mixed = jnp.dot(
                KV[l, slot, 1, :, skip:TOK], PB[h, 0:rows], preferred_element_type=F32
            )
            if slot != 3:
                mixed += MIX[h]
            MIX[h] = mixed
        if slot == 0:
            for h in range(2):
                mixed = (MIX[h] * (1.0 / TOT[h])).astype(BF)
                MX[l, w, 2 * h] = mixed[0:64]
                MX[l, w, 2 * h + 1] = mixed[64:128]
            for i in range(4):
                for piece, step in ((i, (1, 0)), (3 - i, (3, 0)), ((0, 3, 1, 2)[i], (0, 1))):
                    m_to(l, piece, (0, 0), step)
            proj[...] = jnp.zeros_like(proj)

    def kv_event(l, slot):
        if slot == 1:

            @pl.when((y == 0) & (s < NSEQ - 8))
            def _():
                for i in range(2):
                    rows = RB.at[l, pl.ds(32 * i, 32)]
                    arrived(rows, kv_recv.at[l, 3, i])
                    copy(
                        rows, KV.at[l, 1, 1, corner[i]],
                        send.at[l, 11], kv_recv.at[l, 1, 1], on_seq(s + 8),
                    ).start()

            for part in range(2):

                @pl.when(s >= 2)
                def _():
                    arrived(KV.at[l, 1, part], kv_recv.at[l, 1, part])

                @pl.when((core == 0) & (s >= 2))
                def _():
                    kv_far(l, 1, part, here)

                @pl.when((core == 1) & (s >= 2))
                def _():
                    kv_sibling(l, 1, part)

        if slot == 2:

            @pl.when(s >= 1)
            def _():
                for part in range(2):
                    arrived(KV.at[l, 2, part], kv_recv.at[l, 2, part])

        if slot == 0:

            @pl.when(s >= 3)
            def _():
                for part in range(2):
                    arrived(KV.at[l, 0, part, :, late], kv_recv.at[l, 0, part])

    def project(l, first, last):
        def one(group, carry):
            k = group % 4
            index = wgt_of(k * (k + 1) // 2, group // 4)
            block = O[l, pl.ds(8 * index, 8)].reshape(256, WIDTH)
            proj[...] += contract_rows(block, MX[l, index].reshape(256, TOK))
            return carry

        lax.fori_loop(first, last, one, 0)

    def share(l):
        squares = jnp.zeros((1, TOK), F32)
        for i in range(4):
            part = proj[ROWS * i : ROWS * (i + 1)]
            squares += jnp.sum(part * part, axis=0, keepdims=True)
        share_squares(l, 1, squares)

    def finish(l):
        row = lax.rsqrt(all_squares(l, 1) / D + eps)
        for i in range(4):
            post = proj[ROWS * i : ROWS * (i + 1)] * row * gain(l, 1, pl.ds(ROWS * i, ROWS))
            out[i] = (out[i].astype(F32) + post).astype(BF)

    steps = []
    for name in schedule():
        if name[0] in ("mm", "pj"):
            *key, group = name
            if steps and steps[-1][:-2] == tuple(key) and steps[-1][-1] == group:
                steps[-1] = (*steps[-1][:-1], group + 1)
            else:
                steps.append((*key, group, group + 1))
        else:
            steps.append(name)

    for kind, l, *which in steps:
        if kind == "w":
            w_event(l, *which)
        elif kind == "h":
            h_event(l, *which)
        elif kind == "m":
            m_event(l, *which)
        elif kind == "mm":
            multiply(l, *which)
        elif kind == "pj":
            project(l, *which)
        elif kind == "scale":
            scale(l)
        elif kind == "wown":
            w_own(l, (1, 0))
        elif kind == "oown":
            w_own(l, (2, 3))
        elif kind == "hz":
            for i in (0, 3, 1, 2):
                h_to(l, i, (0, 0), (0, 1))
        elif kind == "wsib":
            half = which[0]
            arrived((WA, WB)[half].at[l, pl.ds(0, 16)], sib_recv.at[l, half])
        elif kind == "osib":
            for half in (2, 3):
                arrived(O.at[l, pl.ds(0, 16)], sib_recv.at[l, half])
        elif kind == "kvsent":
            keys_values(l)
        elif kind == "heads":
            queries(l)
        elif kind in ("kv0", "kv1", "kv2"):
            kv_event(l, int(kind[2]))
        elif kind in ("att0", "att1", "att2", "att3"):
            attend(l, int(kind[3]))
        elif kind == "share":
            share(l)
        elif kind == "fin":
            finish(l)

    for l in range(LAYERS):
        sent(WA.at[l, pl.ds(0, 31)], send.at[l, 0])
        sent(WB.at[l, pl.ds(0, 31)], send.at[l, 1])
        sent(O.at[l, pl.ds(0, 31)], send.at[l, 2])
        sent(O.at[l, pl.ds(0, 31)], send.at[l, 3])
        sent(H.at[l, pl.ds(0, 28)], send.at[l, 4])
        sent(MX.at[l, pl.ds(0, 7)], send.at[l, 5])
        for kind in range(2):
            sent(SS.at[l, kind, pl.ds(0, 7)], send.at[l, 6 + kind])

        @pl.when(s < NSEQ - 2)
        def _():
            sent(KV.at[l, 1], send.at[l, 8])

        @pl.when((y == 0) & (s < NSEQ - 8))
        def _():
            sent(RB.at[l], send.at[l, 11])

        @pl.when((core == 0) | (s >= 2))
        def _():
            sent(KV.at[l, 2], send.at[l, 9])

        @pl.when(((core == 0) & (s >= 2)) | ((core == 1) & (s < NSEQ - 3)))
        def _():
            sent(KV.at[l, 0, :, :, late], send.at[l, 10])


def row_factors(scale_codes, first_row, rows):
    blocks = (first_row + jnp.arange(rows, dtype=jnp.int32)) // BLOCK
    pick = blocks[:, None] == jnp.arange(scale_codes.shape[1], dtype=jnp.int32)[None, :]
    factor = jnp.exp2(scale_codes.astype(F32) - 127.0)
    return jnp.sum(jnp.where(pick[None, :, :, None], factor[:, None], 0.0), axis=2)


def per_device(
    hidden,
    q_weight,
    k_weight,
    v_weight,
    o_weight,
    q_scale,
    k_scale,
    v_scale,
    o_scale,
    in_gain,
    post_gain,
    q_gain,
    k_gain,
    windows,
):
    s = lax.axis_index("seq")
    w = lax.axis_index("wgt")
    scales = jnp.concatenate([q_scale, k_scale, v_scale], axis=2)
    factors = jnp.repeat(row_factors(scales, ROWS * s, ROWS), BLOCK, axis=2).astype(BF)
    wa = q_weight * factors[:, :, :256]
    wb = jnp.concatenate([k_weight, v_weight], axis=2) * factors[:, :, 256:]
    o_rows = jnp.exp2(
        lax.dynamic_slice_in_dim(o_scale, s // 2, 1, axis=1).astype(F32) - 127.0
    )
    columns = (w * WIDTH + jnp.arange(WIDTH, dtype=jnp.int32)) // BLOCK
    pick = columns[:, None] == jnp.arange(D // BLOCK, dtype=jnp.int32)[None, :]
    o_factor = jnp.sum(jnp.where(pick[None], o_rows, 0.0), axis=2).astype(BF)
    wo = (o_weight * o_factor[:, None, :]).reshape(LAYERS, 2, 32, WIDTH)
    gin = lax.dynamic_slice_in_dim(in_gain, w * WIDTH, WIDTH, axis=1)
    gains = jnp.concatenate(
        [
            jnp.concatenate([gin, post_gain, jnp.zeros((4, WIDTH), F32)], axis=0),
            jnp.concatenate([q_gain, k_gain, jnp.zeros((4, HD), F32)], axis=0),
        ],
        axis=1,
    ).T
    half = HD // 2
    position = s * TOK + jnp.arange(TOK, dtype=jnp.int32)
    inverse = rope_base ** (-jnp.arange(half, dtype=F32) * 2.0 / HD)
    angles = inverse[:, None] * position.astype(F32)[None, :]
    hid = hidden.T.reshape(4, ROWS, TOK)

    vmem = pl.BlockSpec(memory_space=pltpu.VMEM)
    dma = pltpu.SemaphoreType.DMA
    state = pl.pallas_call(
        kernel,
        out_shape=jax.ShapeDtypeStruct((4, ROWS, TOK), BF),
        in_specs=[vmem] * 7 + [pl.BlockSpec(memory_space=pltpu.SMEM)],
        out_specs=vmem,
        scratch_shapes=[
            pltpu.VMEM((LAYERS, 32, ROWS, TOK), BF),
            pltpu.VMEM((LAYERS, NSEQ, ROWS, 256), BF),
            pltpu.VMEM((LAYERS, NSEQ, ROWS, 256), BF),
            pltpu.VMEM((LAYERS, 2 * NSEQ, 32, WIDTH), BF),
            pltpu.VMEM((LAYERS, NWGT, 4, HD // 2, TOK), BF),
            pltpu.VMEM((LAYERS, 4, 2, HD, TOK), BF),
            pltpu.VMEM((LAYERS, 2, NWGT, 1, TOK), F32),
            pltpu.VMEM((512, TOK), F32),
            pltpu.VMEM((2, HD, TOK), BF),
            pltpu.VMEM((1, TOK), F32),
            pltpu.VMEM((TOK, HD), BF),
            pltpu.VMEM((2, TOK, TOK), F32),
            pltpu.VMEM((2, TOK, TOK), BF),
            pltpu.VMEM((2, 1, TOK), F32),
            pltpu.VMEM((2, HD, TOK), F32),
            pltpu.VMEM((LAYERS, HD // 2, TOK), BF),
            pltpu.VMEM((WIDTH, TOK), F32),
            dma((LAYERS, 2, 4, 4)),
            dma((LAYERS, 2, 4, 4)),
            dma((LAYERS, 4, 2, 4)),
            dma((LAYERS, 4, 2, 4)),
            dma((LAYERS, 4, 2)),
            dma((LAYERS, 4)),
            dma((LAYERS, 2)),
            dma((LAYERS, 12)),
        ],
        compiler_params=pltpu.CompilerParams(
            collective_id=0, has_side_effects=True, vmem_limit_bytes=44 * 1024 * 1024
        ),
    )(
        hid,
        wa,
        wb,
        wo,
        gains,
        jnp.cos(angles),
        jnp.sin(angles),
        windows,
    )
    return state.reshape(WIDTH, TOK).T


def solution(mesh):
    in_specs = (
        P("seq", "wgt"),
        P(None, "seq", "wgt"),
        P(None, "seq", "wgt"),
        P(None, "seq", "wgt"),
        P(None, "seq", "wgt"),
        P(None, None, "wgt"),
        P(None, None, "wgt"),
        P(None, None, "wgt"),
        P(),
        P(),
        P(None, "wgt"),
        P(),
        P(),
        P(),
    )
    return jax.shard_map(
        per_device, mesh=mesh, in_specs=in_specs, out_specs=P("seq", "wgt"), check_vma=False
    )
```

```python
import jax
import jax.numpy as jnp
from jax import lax
from jax.experimental import pallas as pl
from jax.experimental.pallas import tpu as pltpu
from jax.sharding import PartitionSpec as P

HD = 128
BLOCK = 128
LAYERS = 2
NSEQ = 32
NWGT = 8
TOK = 384
WIDTH = 672
ROWS = 168
D = 5376
MESH = pl.DeviceIdType.MESH

eps = 1e-06
query_scale = 168.0 ** (-0.5)
rope_base = 10000.0
BF = jnp.bfloat16
F32 = jnp.float32


def contract_rows(a, b):
    return lax.dot_general(a, b, (((0,), (0,)), ((), ())), preferred_element_type=F32)


Y_US = {"w": 1.9, "o": 1.08, "k": 2.15}
Z_US = {"w": 3.8, "o": 2.15}
X_US = {"h": 2.85, "m": 1.1}
ZP_US = {"h": 2.85, "m": 1.1}
LAT = {"y": 2.2, "z": 2.8, "x": 2.2, "p": 2.2}
H_BY_Z = ((1, 2), (0, 1, 2, 3))


def w_forwards(half, dz, dy):
    first = half in (1, 2)
    steps = []
    if dy == 0:
        if dz == 3 and first:
            steps.append((1, 0))
        if dz == 1 and not first:
            steps.append((3, 0))
        steps += [(0, 1), (0, 3)]
    elif dy == 3 and first:
        steps.append((0, 1))
    elif dy == 1 and not first:
        steps.append((0, 3))
    return steps


def a_forwards(by_z, piece, dx, dz):
    if (dx, dz) == (0, 1):
        return [(1, 0), (3, 0)]
    if (dx, dz) == (2, 0):
        return [(0, 1)] if piece in by_z else []
    if dz == 1 and piece in by_z:
        return []
    if dx == 3 and piece < 2:
        return [(1, 0)]
    if dx == 1 and piece >= 2:
        return [(3, 0)]
    return []


M_BY_Z = ((1, 2), (1, 2))
BY_Z = {"h": H_BY_Z, "m": M_BY_Z}


SLACK = ((0.5, 1.0), (4.0, 4.0))


def schedule():
    free = {}
    arrival = {}
    done = {}
    order = []
    now = 0.0

    def link(name, us, lat):
        free[name] = max(free.get(name, 0.0), now) + us
        return free[name] + lat

    def send_w(l, half, rel, step):
        kind = "w" if half < 2 else "o"
        to = ((rel[0] - step[0]) % 4, (rel[1] - step[1]) % 4)
        if step[0]:
            t = link("z" + str(step[0]), Z_US[kind], LAT["z"])
        else:
            t = link("y" + str(step[1]), Y_US[kind], LAT["y"])
        arrival["w", l, half, *to] = t

    def send_a(kind, l, piece, rel, step):
        to = ((rel[0] - step[0]) % 4, (rel[1] - step[1]) % 2)
        if step[0]:
            t = link("x" + str(step[0]), X_US[kind], LAT["x"])
        else:
            t = link("z1", ZP_US[kind], LAT["p"])
        arrival[kind, l, piece, *to] = t

    w_events = lambda l, half0: [("w", l, h, dz, dy) for h in (half0, half0 + 1) for dz in range(4) for dy in range(4) if (dz, dy) != (0, 0)]
    owner = lambda g: ([0, 1, 3, 2][g % 4], g // 4)

    tasks = {}
    for l in range(2):
        tasks["scale", l] = (0.3, [("fin", 0)] if l else [("wown", 0)], 0)
        tasks["wown", l] = (0.05, [("att0", 0)] if l else [], 1)
        tasks["oown", l] = (0.05, ([("scale", 1)] if l else []) + [("w", l, h, dz, 0) for h in (0, 1) for dz in (1, 2, 3)], 1)
        tasks["hz", l] = (0.05, [("scale", l)] + [("w", l, h, dz, 0) for h in (0, 1) for dz in (1, 3)], 0)
        for half in (0, 1):
            name = ("wsib", l, half)
            tasks[name] = (0.02, [e for e in w_events(l, 0) if e[2] == half] + [("kvsent", 0) if (l, half) == (0, 0) else ("scale", l)], 2 - half)
            for g in range(8):
                ow = owner(g)
                pieces = [("scale", l)] if ow == (0, 0) else [("h", l, i, *ow) for i in range(4)]
                tasks["mm", l, half, g] = (0.45, [name] + pieces, 4 - half)
        tasks["kvsent", l] = (0.15, [("mm", l, 1, g) for g in range(8)], 0)
        tasks["heads", l] = (0.2, [("mm", l, 0, g) for g in range(8)] + [("kvsent", l)], 1)
        tasks["att3", l] = (1.07, [("heads", l)], 3)
        tasks["att1", l] = (1.12, [("att3", l), ("kv1", l)], 3)
        tasks["att2", l] = (1.12, [("att1", l), ("kv2", l)], 3)
        tasks["att0", l] = (1.1, [("att2", l), ("kv0", l)], 0)
        tasks["osib", l] = (0.02, w_events(l, 2) + [("att0", l)], 2)
        for g in range(8):
            ow = owner(g)
            tasks["pj", l, g] = (0.38, [("osib", l), ("att0", l)] + ([] if ow == (0, 0) else [("m", l, i, *ow) for i in range(4)]), 3)
        tasks["share", l] = (0.3, [("pj", l, g) for g in range(8)], 0)
        tasks["fin", l] = (0.3, [("share", l), ("ss", l)], 0)

    def run_task(name):
        nonlocal now
        kind, l = name[0], name[1]
        now += tasks[name][0]
        if kind == "wown":
            for h in (1, 0):
                for step in ((0, 1), (0, 3), (1, 0), (3, 0)):
                    send_w(l, h, (0, 0), step)
        if kind == "oown":
            for h in (2, 3):
                for step in ((0, 1), (0, 3), (1, 0), (3, 0)):
                    send_w(l, h, (0, 0), step)
        if kind == "scale":
            for i in range(4):
                send_a("h", l, i, (0, 0), (1, 0))
                send_a("h", l, 3 - i, (0, 0), (3, 0))
        if kind == "hz":
            for i in (0, 3, 1, 2):
                send_a("h", l, i, (0, 0), (0, 1))
        if kind == "kvsent":
            a = link("y1", Y_US["k"], 2.8)
            b = link("y1", Y_US["k"], 2.8)
            arrival["kv1", l] = b + 0.5
            arrival["kv2", l] = b + 2.3
            arrival["kv0", l] = b + 2.5
        if kind == "att0":
            for i in range(4):
                for piece, step in ((i, (1, 0)), (3 - i, (3, 0)), ((0, 3, 1, 2)[i], (0, 1))):
                    send_a("m", l, piece, (0, 0), step)
        if kind == "share":
            arrival["ss", l] = now + 4.0
        done[name] = now
        order.append(name)

    def run_event(ev):
        nonlocal now
        now += 0.06
        kind = ev[0]
        if kind == "w":
            _, l, half, dz, dy = ev
            for step in w_forwards(half, dz, dy):
                send_w(l, half, (dz, dy), step)
        elif kind in "hm":
            _, l, piece, dx, dz = ev
            for step in a_forwards(BY_Z[kind][l], piece, dx, dz):
                send_a(kind, l, piece, (dx, dz), step)
        done[ev] = now
        order.append(ev)

    def eff(ev):
        t = arrival[ev]
        if ev[0] == "w":
            return t + SLACK[ev[1]][ev[2] // 2]
        if ev[0] in "hm" and ev[3:] == (0, 1):
            return t + 0.5
        return t

    while True:
        pend = [e for e in arrival if e not in done]
        ready = [t for t in tasks if t not in done and all(d in done for d in tasks[t][1])]
        if not pend and not ready:
            break
        urgent = [t for t in ready if tasks[t][2] == 0]
        arrived = [e for e in pend if eff(e) <= now]
        if urgent:
            run_task(min(urgent))
        elif arrived:
            run_event(min(arrived, key=lambda e: (eff(e), e)))
        elif ready:
            run_task(min(ready, key=lambda t: (tasks[t][2], tasks[t][1] and max(done[d] for d in tasks[t][1]) or 0, t)))
        else:
            e = min(pend, key=lambda e: (eff(e), e))
            now = max(now, eff(e))
            run_event(e)
    return order


def kernel(
    hid, wq, wk, wv, wo, factors, o_factors, gains, cosine, sine, windows,
    out,
    H, WA, WB, O, MX, KV, SS, acc, Q, ROW, KX, SC, PB, TOT, MIX, RB, proj,
    w_recv, o_recv, h_recv, mx_recv, kv_recv, sib_recv, ss_recv, send,
):
    s = lax.axis_index("seq")
    w = lax.axis_index("wgt")
    core = s % 2
    y = (s // 2) % 4
    zh = s // 8
    x = w // 2
    zl = w % 2

    def seq_of(dz, dy):
        return ((zh + dz) % 4) * 8 + ((y + dy) % 4) * 2 + core

    def wgt_of(dx, dz):
        return ((x + dx) % 4) * 2 + (zl + dz) % 2

    sibling = s + 1 - 2 * core

    def on_seq(i):
        return {"seq": i, "wgt": w}

    def on_wgt(i):
        return {"seq": s, "wgt": i}

    def copy(src, dst, send_sem, recv_sem, device):
        return pltpu.make_async_remote_copy(
            src_ref=src,
            dst_ref=dst,
            send_sem=send_sem,
            recv_sem=recv_sem,
            device_id=device,
            device_id_type=MESH,
        )

    here = on_seq(sibling)

    def arrived(dst, sem):
        copy(dst, dst, send.at[0, 0], sem, here).wait_recv()

    def sent(region, sem):
        copy(region, region, sem, w_recv.at[0, 0, 0, 0], here).wait_send()

    def w_slot(l, half, index):
        if half == 0:
            return WA.at[l, index]
        if half == 1:
            return WB.at[l, index]
        return O.at[l, 2 * index + (half - 2)]

    def w_sem(l, half, dz, dy):
        if half < 2:
            return w_recv.at[l, half, dz, dy]
        return o_recv.at[l, half - 2, dz, dy]

    def w_to(l, half, owner, rel, step):
        slot = w_slot(l, half, owner)
        to = ((rel[0] - step[0]) % 4, (rel[1] - step[1]) % 4)
        copy(
            slot, slot, send.at[l, half], w_sem(l, half, *to), on_seq(seq_of(*step))
        ).start()

    def w_to_sibling(l, half, owner):
        slot = w_slot(l, half, owner)
        copy(slot, slot, send.at[l, half], sib_recv.at[l, half], here).start()

    def w_own(l, halves, along="yz"):
        for half in halves:
            if "y" in along:
                w_to(l, half, s, (0, 0), (0, 1))
                w_to(l, half, s, (0, 0), (0, 3))
                w_to_sibling(l, half, s)
            if "z" in along:
                w_to(l, half, s, (0, 0), (1, 0))
                w_to(l, half, s, (0, 0), (3, 0))

    def w_event(l, half, dz, dy):
        owner = seq_of(dz, dy)
        arrived(w_slot(l, half, owner), w_sem(l, half, dz, dy))
        for step in w_forwards(half, dz, dy):
            w_to(l, half, owner, (dz, dy), step)
        w_to_sibling(l, half, owner)

    def h_to(l, piece, rel, step):
        slot = H.at[l, 4 * wgt_of(*rel) + piece]
        to = ((rel[0] - step[0]) % 4, (rel[1] - step[1]) % 2)
        copy(
            slot, slot, send.at[l, 4], h_recv.at[l, to[0], to[1], piece], on_wgt(wgt_of(*step))
        ).start()

    def m_to(l, piece, rel, step):
        slot = MX.at[l, wgt_of(*rel), piece]
        to = ((rel[0] - step[0]) % 4, (rel[1] - step[1]) % 2)
        copy(
            slot, slot, send.at[l, 5], mx_recv.at[l, to[0], to[1], piece], on_wgt(wgt_of(*step))
        ).start()

    def h_event(l, piece, dx, dz):
        arrived(H.at[l, 4 * wgt_of(dx, dz) + piece], h_recv.at[l, dx, dz, piece])
        for step in a_forwards(BY_Z["h"][l], piece, dx, dz):
            h_to(l, piece, (dx, dz), step)

    def m_event(l, piece, dx, dz):
        arrived(MX.at[l, wgt_of(dx, dz), piece], mx_recv.at[l, dx, dz, piece])
        for step in a_forwards(BY_Z["m"][l], piece, dx, dz):
            m_to(l, piece, (dx, dz), step)

    peers = [(dx, dz) for dz in range(2) for dx in range(4) if (dx, dz) != (0, 0)]

    def share_squares(l, kind, row):
        SS[l, kind, w] = row
        slot = SS.at[l, kind, w]
        for rel in peers:
            copy(
                slot, slot, send.at[l, 6 + kind], ss_recv.at[l, kind], on_wgt(wgt_of(*rel))
            ).start()

    def all_squares(l, kind):
        arrived(SS.at[l, kind, pl.ds(0, 7)], ss_recv.at[l, kind])
        return jnp.sum(SS[l, kind], axis=0)

    def gain(l, kind, rows):
        return gains[rows, 2 * kind + l : 2 * kind + l + 1]

    def dequantize(l):
        for j, (dst, src) in enumerate(
            (
                (WA.at[l, s, :, 0:128], wq.at[l, :, 0:128]),
                (WA.at[l, s, :, 128:256], wq.at[l, :, 128:256]),
                (WB.at[l, s, :, 0:128], wk.at[l]),
                (WB.at[l, s, :, 128:256], wv.at[l]),
            )
        ):
            dst[...] = src[...] * factors[l, :, j : j + 1]
        for half in range(2):
            O[l, 2 * s + half] = wo[l, 32 * half : 32 * half + 32] * o_factors[l : l + 1]

    dequantize(0)
    for l in range(LAYERS):
        for slot in range(3):
            KV[l, slot] = jnp.zeros((2, HD, TOK), BF)

    barrier = pltpu.get_barrier_semaphore()
    neighbours = [here]
    neighbours += [on_seq(seq_of(*step)) for step in ((0, 1), (0, 3), (1, 0), (3, 0))]
    neighbours += [on_wgt(wgt_of(*rel)) for rel in peers]
    after = on_seq((s + 2) % NSEQ)
    neighbours += [after, on_seq((s + NSEQ - 2) % NSEQ)]
    neighbours += [on_seq((s + NSEQ - 3 + 6 * core) % NSEQ)]
    for device in neighbours:
        pl.semaphore_signal(barrier, inc=1, device_id=device, device_id_type=MESH)
    pl.semaphore_wait(barrier, len(neighbours))

    late = pl.ds(128, 256)

    def scale(l):
        row = lax.rsqrt(all_squares(l - 1, 1) / D + eps) if l else None
        squares = jnp.zeros((1, TOK), F32)
        for i in (0, 3, 1, 2):
            if l == 0:
                out[i] = hid[i]
                state = hid[i].astype(F32)
            else:
                out[i] = next_state(l - 1, i, row)
                state = out[i].astype(F32)
            H[l, 4 * w + i] = (state * gain(l, 0, pl.ds(ROWS * i, ROWS))).astype(BF)
            squares += jnp.sum(state * state, axis=0, keepdims=True)
            h_to(l, i, (0, 0), (1, 0) if i < 2 else (3, 0))
        for i in (2, 3):
            h_to(l, i, (0, 0), (1, 0))
            h_to(l, 3 - i, (0, 0), (3, 0))
        share_squares(l, 0, squares)
        acc[...] = jnp.zeros_like(acc)
    def multiply(l, half, first, last):
        buf, rows = ((WA, pl.ds(0, 256)), (WB, pl.ds(256, 256)))[half]

        def one(group, carry):
            k = group % 4
            index = 4 * wgt_of(k * (k + 1) // 2, group // 4)
            total = acc[rows]
            for i in range(4):
                total += contract_rows(buf[l, index + i], H[l, index + i])
            acc[rows] = total
            return carry

        lax.fori_loop(first, last, one, 0)

    def head_of(l, rows, row, kind):
        values = acc[rows] * row
        values *= lax.rsqrt(jnp.mean(values * values, axis=0, keepdims=True) + eps)
        values *= gain(l, kind, pl.ds(WIDTH, HD))
        first = values[0:64]
        second = values[64:128]
        c = cosine[...]
        n = sine[...]
        return first * c - second * n, second * c + first * n

    def kv_sibling(l, slot, part):
        copy(
            KV.at[l, slot, part], KV.at[l, 2, part],
            send.at[l, 9], kv_recv.at[l, 2, part], here,
        ).start()

    def kv_far(l, slot, part, device):
        copy(
            KV.at[l, slot, part, :, late], KV.at[l, 0, part, :, late],
            send.at[l, 10], kv_recv.at[l, 0, part], device,
        ).start()

    def kv_next(l, part, rows):
        copy(
            KV.at[l, 3, part, rows], KV.at[l, 1, part, rows],
            send.at[l, 8], kv_recv.at[l, 1, part], after,
        ).start()

    corner = [pl.ds(64 + 32 * i, 32) for i in range(2)]

    def keys_values(l):
        row = lax.rsqrt(all_squares(l, 0) / D + eps)
        ROW[...] = row
        KV[l, 3, 1] = (acc[384:512] * row).astype(BF)

        @pl.when((y == 3) & (s < NSEQ - 2))
        def _():
            for i in range(2):
                copy(
                    KV.at[l, 3, 1, corner[i]], RB.at[l, pl.ds(32 * i, 32)],
                    send.at[l, 8], kv_recv.at[l, 3, i], on_seq(s - 6),
                ).start()

        first, second = head_of(l, pl.ds(256, 128), row, 1)
        KV[l, 3, 0, 0:64] = first.astype(BF)
        KV[l, 3, 0, 64:128] = second.astype(BF)

        @pl.when(s < NSEQ - 2)
        def _():
            kv_next(l, 0, pl.ds(0, 128))
            kv_next(l, 1, pl.ds(0, 64))

        @pl.when((y != 3) & (s < NSEQ - 2))
        def _():
            kv_next(l, 1, pl.ds(64, 64))

        @pl.when(core == 0)
        def _():
            for part in range(2):
                kv_sibling(l, 3, part)

        @pl.when((core == 1) & (s < NSEQ - 3))
        def _():
            for part in range(2):
                kv_far(l, 3, part, on_seq((s + 3) % NSEQ))

    def queries(l):
        for h in range(2):
            first, second = head_of(l, pl.ds(128 * h, 128), ROW[...], 0)
            Q[h, 0:64] = (first * query_scale).astype(BF)
            Q[h, 64:128] = (second * query_scale).astype(BF)

    def attend(l, slot):
        skip = 128 if slot == 0 else 0
        rows = TOK - skip
        window = windows[l]
        KX[0:rows] = KV[l, slot, 0, :, skip:TOK].T
        keys = lax.broadcasted_iota(jnp.int32, (rows, 128), 0) + (TOK * slot + skip)
        for h in range(2):
            SC[h, 0:rows] = jnp.dot(KX[0:rows], Q[h], preferred_element_type=F32)
        for h in range(2):
            for c in range(3):
                lanes = pl.ds(128 * c, 128)
                gap = lax.broadcasted_iota(jnp.int32, (rows, 128), 1) + (128 * c + 3 * TOK) - keys
                allowed = (gap < window) & (keys >= 3 * TOK - TOK * s)
                if slot == 3:
                    allowed &= gap >= 0
                weight = jnp.where(allowed, jnp.exp(SC[h, 0:rows, lanes]), 0.0)
                total = jnp.sum(weight, axis=0, keepdims=True)
                if slot != 3:
                    total += TOT[h, :, lanes]
                TOT[h, :, lanes] = total
                PB[h, 0:rows, lanes] = weight.astype(BF)
            mixed = jnp.dot(
                KV[l, slot, 1, :, skip:TOK], PB[h, 0:rows], preferred_element_type=F32
            )
            if slot != 3:
                mixed += MIX[h]
            MIX[h] = mixed
        if slot == 0:
            for h in range(2):
                mixed = (MIX[h] * (1.0 / TOT[h])).astype(BF)
                MX[l, w, 2 * h] = mixed[0:64]
                MX[l, w, 2 * h + 1] = mixed[64:128]
            for i in range(4):
                for piece, step in ((i, (1, 0)), (3 - i, (3, 0)), ((0, 3, 1, 2)[i], (0, 1))):
                    m_to(l, piece, (0, 0), step)
            proj[...] = jnp.zeros_like(proj)

    def kv_event(l, slot):
        if slot == 1:

            @pl.when((y == 0) & (s < NSEQ - 8))
            def _():
                for i in range(2):
                    rows = RB.at[l, pl.ds(32 * i, 32)]
                    arrived(rows, kv_recv.at[l, 3, i])
                    copy(
                        rows, KV.at[l, 1, 1, corner[i]],
                        send.at[l, 11], kv_recv.at[l, 1, 1], on_seq(s + 8),
                    ).start()

            for part in range(2):

                @pl.when(s >= 2)
                def _():
                    arrived(KV.at[l, 1, part], kv_recv.at[l, 1, part])

                @pl.when((core == 0) & (s >= 2))
                def _():
                    kv_far(l, 1, part, here)

                @pl.when((core == 1) & (s >= 2))
                def _():
                    kv_sibling(l, 1, part)

        if slot == 2:

            @pl.when(s >= 1)
            def _():
                for part in range(2):
                    arrived(KV.at[l, 2, part], kv_recv.at[l, 2, part])

        if slot == 0:

            @pl.when(s >= 3)
            def _():
                for part in range(2):
                    arrived(KV.at[l, 0, part, :, late], kv_recv.at[l, 0, part])

    def project(l, first, last):
        def one(group, carry):
            k = group % 4
            index = wgt_of(k * (k + 1) // 2, group // 4)
            block = O[l, pl.ds(8 * index, 8)].reshape(256, WIDTH)
            proj[...] += contract_rows(block, MX[l, index].reshape(256, TOK))
            return carry

        lax.fori_loop(first, last, one, 0)

    def share(l):
        squares = jnp.zeros((1, TOK), F32)
        for i in range(4):
            part = proj[ROWS * i : ROWS * (i + 1)]
            squares += jnp.sum(part * part, axis=0, keepdims=True)
        share_squares(l, 1, squares)

    def next_state(l, i, row):
        rows = pl.ds(ROWS * i, ROWS)
        post = proj[rows] * row * gain(l, 1, rows)
        return (out[i].astype(F32) + post).astype(BF)

    def finish(l):
        if l == LAYERS - 1:
            row = lax.rsqrt(all_squares(l, 1) / D + eps)
            for i in range(4):
                out[i] = next_state(l, i, row)

    steps = []
    for name in schedule():
        if name[0] in ("mm", "pj"):
            *key, group = name
            if steps and steps[-1][:-2] == tuple(key) and steps[-1][-1] == group:
                steps[-1] = (*steps[-1][:-1], group + 1)
            else:
                steps.append((*key, group, group + 1))
        else:
            steps.append(name)

    for kind, l, *which in steps:
        if kind == "w":
            w_event(l, *which)
        elif kind == "h":
            h_event(l, *which)
        elif kind == "m":
            m_event(l, *which)
        elif kind == "mm":
            multiply(l, *which)
        elif kind == "pj":
            project(l, *which)
        elif kind == "scale":
            scale(l)
        elif kind == "wown":
            w_own(l, (1, 0))
        elif kind == "oown":
            w_own(l, (2, 3))
        elif kind == "hz":
            for i in (0, 3, 1, 2):
                h_to(l, i, (0, 0), (0, 1))
            if l == 0:
                dequantize(1)
        elif kind == "wsib":
            half = which[0]
            arrived((WA, WB)[half].at[l, pl.ds(0, 16)], sib_recv.at[l, half])
        elif kind == "osib":
            for half in (2, 3):
                arrived(O.at[l, pl.ds(0, 16)], sib_recv.at[l, half])
        elif kind == "kvsent":
            keys_values(l)
        elif kind == "heads":
            queries(l)
        elif kind in ("kv0", "kv1", "kv2"):
            kv_event(l, int(kind[2]))
        elif kind in ("att0", "att1", "att2", "att3"):
            attend(l, int(kind[3]))
        elif kind == "share":
            share(l)
        elif kind == "fin":
            finish(l)

    for l in range(LAYERS):
        sent(WA.at[l, pl.ds(0, 31)], send.at[l, 0])
        sent(WB.at[l, pl.ds(0, 31)], send.at[l, 1])
        sent(O.at[l, pl.ds(0, 31)], send.at[l, 2])
        sent(O.at[l, pl.ds(0, 31)], send.at[l, 3])
        sent(H.at[l, pl.ds(0, 28)], send.at[l, 4])
        sent(MX.at[l, pl.ds(0, 7)], send.at[l, 5])
        for kind in range(2):
            sent(SS.at[l, kind, pl.ds(0, 7)], send.at[l, 6 + kind])

        @pl.when(s < NSEQ - 2)
        def _():
            sent(KV.at[l, 1], send.at[l, 8])

        @pl.when((y == 0) & (s < NSEQ - 8))
        def _():
            sent(RB.at[l], send.at[l, 11])

        @pl.when((core == 0) | (s >= 2))
        def _():
            sent(KV.at[l, 2], send.at[l, 9])

        @pl.when(((core == 0) & (s >= 2)) | ((core == 1) & (s < NSEQ - 3)))
        def _():
            sent(KV.at[l, 0, :, :, late], send.at[l, 10])


def row_factors(scale_codes, first_row, rows):
    blocks = (first_row + jnp.arange(rows, dtype=jnp.int32)) // BLOCK
    pick = blocks[:, None] == jnp.arange(scale_codes.shape[1], dtype=jnp.int32)[None, :]
    factor = jnp.exp2(scale_codes.astype(F32) - 127.0)
    return jnp.sum(jnp.where(pick[None, :, :, None], factor[:, None], 0.0), axis=2)


def per_device(
    hidden,
    q_weight,
    k_weight,
    v_weight,
    o_weight,
    q_scale,
    k_scale,
    v_scale,
    o_scale,
    in_gain,
    post_gain,
    q_gain,
    k_gain,
    windows,
):
    s = lax.axis_index("seq")
    w = lax.axis_index("wgt")
    scales = jnp.concatenate([q_scale, k_scale, v_scale], axis=2)
    factors = row_factors(scales, ROWS * s, ROWS).astype(BF)
    o_rows = jnp.exp2(
        lax.dynamic_slice_in_dim(o_scale, s // 2, 1, axis=1).astype(F32) - 127.0
    )
    columns = (w * WIDTH + jnp.arange(WIDTH, dtype=jnp.int32)) // BLOCK
    pick = columns[:, None] == jnp.arange(D // BLOCK, dtype=jnp.int32)[None, :]
    o_factor = jnp.sum(jnp.where(pick[None], o_rows, 0.0), axis=2).astype(BF)
    gin = lax.dynamic_slice_in_dim(in_gain, w * WIDTH, WIDTH, axis=1)
    gains = jnp.concatenate(
        [
            jnp.concatenate([gin, post_gain, jnp.zeros((4, WIDTH), F32)], axis=0),
            jnp.concatenate([q_gain, k_gain, jnp.zeros((4, HD), F32)], axis=0),
        ],
        axis=1,
    ).T
    half = HD // 2
    position = s * TOK + jnp.arange(TOK, dtype=jnp.int32)
    inverse = rope_base ** (-jnp.arange(half, dtype=F32) * 2.0 / HD)
    angles = inverse[:, None] * position.astype(F32)[None, :]
    hid = hidden.T.reshape(4, ROWS, TOK)

    vmem = pl.BlockSpec(memory_space=pltpu.VMEM)
    dma = pltpu.SemaphoreType.DMA
    state = pl.pallas_call(
        kernel,
        out_shape=jax.ShapeDtypeStruct((4, ROWS, TOK), BF),
        in_specs=[vmem] * 10 + [pl.BlockSpec(memory_space=pltpu.SMEM)],
        out_specs=vmem,
        scratch_shapes=[
            pltpu.VMEM((LAYERS, 32, ROWS, TOK), BF),
            pltpu.VMEM((LAYERS, NSEQ, ROWS, 256), BF),
            pltpu.VMEM((LAYERS, NSEQ, ROWS, 256), BF),
            pltpu.VMEM((LAYERS, 2 * NSEQ, 32, WIDTH), BF),
            pltpu.VMEM((LAYERS, NWGT, 4, HD // 2, TOK), BF),
            pltpu.VMEM((LAYERS, 4, 2, HD, TOK), BF),
            pltpu.VMEM((LAYERS, 2, NWGT, 1, TOK), F32),
            pltpu.VMEM((512, TOK), F32),
            pltpu.VMEM((2, HD, TOK), BF),
            pltpu.VMEM((1, TOK), F32),
            pltpu.VMEM((TOK, HD), BF),
            pltpu.VMEM((2, TOK, TOK), F32),
            pltpu.VMEM((2, TOK, TOK), BF),
            pltpu.VMEM((2, 1, TOK), F32),
            pltpu.VMEM((2, HD, TOK), F32),
            pltpu.VMEM((LAYERS, HD // 2, TOK), BF),
            pltpu.VMEM((WIDTH, TOK), F32),
            dma((LAYERS, 2, 4, 4)),
            dma((LAYERS, 2, 4, 4)),
            dma((LAYERS, 4, 2, 4)),
            dma((LAYERS, 4, 2, 4)),
            dma((LAYERS, 4, 2)),
            dma((LAYERS, 4)),
            dma((LAYERS, 2)),
            dma((LAYERS, 12)),
        ],
        compiler_params=pltpu.CompilerParams(
            collective_id=0, has_side_effects=True, vmem_limit_bytes=44 * 1024 * 1024
        ),
    )(
        hid,
        q_weight,
        k_weight,
        v_weight,
        o_weight,
        factors,
        o_factor,
        gains,
        jnp.cos(angles),
        jnp.sin(angles),
        windows,
    )
    return state.reshape(WIDTH, TOK).T


def solution(mesh):
    in_specs = (
        P("seq", "wgt"),
        P(None, "seq", "wgt"),
        P(None, "seq", "wgt"),
        P(None, "seq", "wgt"),
        P(None, "seq", "wgt"),
        P(None, None, "wgt"),
        P(None, None, "wgt"),
        P(None, None, "wgt"),
        P(),
        P(),
        P(None, "wgt"),
        P(),
        P(),
        P(),
    )
    return jax.shard_map(
        per_device, mesh=mesh, in_specs=in_specs, out_specs=P("seq", "wgt"), check_vma=False
    )
```

```python
import jax
import jax.numpy as jnp
from jax import lax
from jax.experimental import pallas as pl
from jax.experimental.pallas import tpu as pltpu
from jax.sharding import PartitionSpec as P

HD = 128
BLOCK = 128
LAYERS = 2
NSEQ = 32
NWGT = 8
TOK = 384
WIDTH = 672
ROWS = 168
D = 5376
MESH = pl.DeviceIdType.MESH

eps = 1e-06
query_scale = 168.0 ** (-0.5)
rope_base = 10000.0
BF = jnp.bfloat16
F32 = jnp.float32


def contract_rows(a, b):
    return lax.dot_general(a, b, (((0,), (0,)), ((), ())), preferred_element_type=F32)


Y_US = {"w": 1.9, "o": 1.08, "k": 2.15}
Z_US = {"w": 3.8, "o": 2.15}
X_US = {"h": 2.85, "m": 1.1}
ZP_US = {"h": 2.85, "m": 1.1}
LAT = {"y": 2.2, "z": 2.8, "x": 2.2, "p": 2.2}
H_BY_Z = ((1, 2), (0, 1, 2, 3))


def w_forwards(half, dz, dy):
    first = half in (1, 2)
    steps = []
    if dy == 0:
        if dz == 3 and first:
            steps.append((1, 0))
        if dz == 1 and not first:
            steps.append((3, 0))
        steps += [(0, 1), (0, 3)]
    elif dy == 3 and first:
        steps.append((0, 1))
    elif dy == 1 and not first:
        steps.append((0, 3))
    return steps


def a_forwards(by_z, piece, dx, dz):
    if (dx, dz) == (0, 1):
        return [(1, 0), (3, 0)]
    if (dx, dz) == (2, 0):
        return [(0, 1)] if piece in by_z else []
    if dz == 1 and piece in by_z:
        return []
    if dx == 3 and piece < 2:
        return [(1, 0)]
    if dx == 1 and piece >= 2:
        return [(3, 0)]
    return []


M_BY_Z = ((1, 2), (1, 2))
BY_Z = {"h": H_BY_Z, "m": M_BY_Z}


SLACK = ((0.5, 3.0), (6.0, 5.0))


def schedule():
    free = {}
    arrival = {}
    done = {}
    order = []
    now = 0.0

    def link(name, us, lat):
        free[name] = max(free.get(name, 0.0), now) + us
        return free[name] + lat

    def send_w(l, half, rel, step):
        kind = "w" if half < 2 else "o"
        to = ((rel[0] - step[0]) % 4, (rel[1] - step[1]) % 4)
        if step[0]:
            t = link("z" + str(step[0]), Z_US[kind], LAT["z"])
        else:
            t = link("y" + str(step[1]), Y_US[kind], LAT["y"])
        arrival["w", l, half, *to] = t

    def send_a(kind, l, piece, rel, step):
        to = ((rel[0] - step[0]) % 4, (rel[1] - step[1]) % 2)
        if step[0]:
            t = link("x" + str(step[0]), X_US[kind], LAT["x"])
        else:
            t = link("z1", ZP_US[kind], LAT["p"])
        arrival[kind, l, piece, *to] = t

    w_events = lambda l, half0: [("w", l, h, dz, dy) for h in (half0, half0 + 1) for dz in range(4) for dy in range(4) if (dz, dy) != (0, 0)]
    owner = lambda g: ([0, 1, 3, 2][g % 4], g // 4)

    tasks = {}
    for l in range(2):
        tasks["scale", l] = (0.3, [("fin", 0)] if l else [("wown", 0)], 0)
        tasks["wown", l] = (0.05, [("att0", 0)] if l else [], 1)
        tasks["oown", l] = (0.05, ([("scale", 1)] if l else []) + [("w", l, h, dz, 0) for h in (0, 1) for dz in (1, 2, 3)], 1)
        tasks["hz", l] = (0.05, [("scale", l)] + [("w", l, h, dz, 0) for h in (0, 1) for dz in (1, 3)], 0)
        for half in (0, 1):
            name = ("wsib", l, half)
            tasks[name] = (0.02, [e for e in w_events(l, 0) if e[2] == half] + [("kvsent", 0) if (l, half) == (0, 0) else ("scale", l)], 2 - half)
            for g in range(8):
                ow = owner(g)
                pieces = [("scale", l)] if ow == (0, 0) else [("h", l, i, *ow) for i in range(4)]
                tasks["mm", l, half, g] = (0.45, [name] + pieces, 4 - half)
        tasks["kvsent", l] = (0.15, [("mm", l, 1, g) for g in range(8)], 0)
        tasks["heads", l] = (0.2, [("mm", l, 0, g) for g in range(8)] + [("kvsent", l)], 1)
        tasks["att3", l] = (1.07, [("heads", l)], 3)
        tasks["att1", l] = (1.12, [("att3", l), ("kv1", l)], 3)
        tasks["att2", l] = (1.12, [("att1", l), ("kv2", l)], 3)
        tasks["att0", l] = (1.1, [("att2", l), ("kv0", l)], 0)
        tasks["osib", l] = (0.02, w_events(l, 2) + [("att0", l)], 2)
        for g in range(8):
            ow = owner(g)
            tasks["pj", l, g] = (0.38, [("osib", l), ("att0", l)] + ([] if ow == (0, 0) else [("m", l, i, *ow) for i in range(4)]), 3)
        tasks["share", l] = (0.3, [("pj", l, g) for g in range(8)], 0)
        tasks["fin", l] = (0.3, [("share", l), ("ss", l)], 0)

    def run_task(name):
        nonlocal now
        kind, l = name[0], name[1]
        now += tasks[name][0]
        if kind == "wown":
            for h in (1, 0):
                for step in ((0, 1), (0, 3), (1, 0), (3, 0)):
                    send_w(l, h, (0, 0), step)
        if kind == "oown":
            for h in (2, 3):
                for step in ((0, 1), (0, 3), (1, 0), (3, 0)):
                    send_w(l, h, (0, 0), step)
        if kind == "scale":
            for i in range(4):
                send_a("h", l, i, (0, 0), (1, 0))
                send_a("h", l, 3 - i, (0, 0), (3, 0))
        if kind == "hz":
            for i in (0, 3, 1, 2):
                send_a("h", l, i, (0, 0), (0, 1))
        if kind == "kvsent":
            a = link("y1", Y_US["k"], 2.8)
            b = link("y1", Y_US["k"], 2.8)
            arrival["kv1", l] = b + 0.5
            arrival["kv2", l] = b + 2.3
            arrival["kv0", l] = b + 2.5
        if kind == "att0":
            for i in range(4):
                for piece, step in ((i, (1, 0)), (3 - i, (3, 0)), ((0, 3, 1, 2)[i], (0, 1))):
                    send_a("m", l, piece, (0, 0), step)
        if kind == "share":
            arrival["ss", l] = now + 4.0
        done[name] = now
        order.append(name)

    def run_event(ev):
        nonlocal now
        now += 0.06
        kind = ev[0]
        if kind == "w":
            _, l, half, dz, dy = ev
            for step in w_forwards(half, dz, dy):
                send_w(l, half, (dz, dy), step)
        elif kind in "hm":
            _, l, piece, dx, dz = ev
            for step in a_forwards(BY_Z[kind][l], piece, dx, dz):
                send_a(kind, l, piece, (dx, dz), step)
        done[ev] = now
        order.append(ev)

    def eff(ev):
        t = arrival[ev]
        if ev[0] == "w":
            slack = SLACK[ev[1]][ev[2] // 2]
            return t + (min(slack, 4.0) if ("scale", 1) in done else slack)
        if ev[0] in "hm" and ev[3:] == (0, 1):
            return t + 0.5
        return t

    while True:
        pend = [e for e in arrival if e not in done]
        ready = [t for t in tasks if t not in done and all(d in done for d in tasks[t][1])]
        if not pend and not ready:
            break
        urgent = [t for t in ready if tasks[t][2] == 0]
        arrived = [e for e in pend if eff(e) <= now]
        if urgent:
            run_task(min(urgent))
        elif arrived:
            run_event(min(arrived, key=lambda e: (eff(e), e)))
        elif ready:
            run_task(min(ready, key=lambda t: (tasks[t][2], tasks[t][1] and max(done[d] for d in tasks[t][1]) or 0, t)))
        else:
            e = min(pend, key=lambda e: (eff(e), e))
            now = max(now, eff(e))
            run_event(e)
    return order


def kernel(
    hid, wq, wk, wv, wo, factors, o_factors, gains, cosine, sine, windows,
    out,
    H, WA, WB, O, MX, KV, SS, acc, Q, ROW, KX, SC, PB, TOT, MIX, RB, proj,
    w_recv, o_recv, h_recv, mx_recv, kv_recv, sib_recv, ss_recv, send,
):
    s = lax.axis_index("seq")
    w = lax.axis_index("wgt")
    core = s % 2
    y = (s // 2) % 4
    zh = s // 8
    x = w // 2
    zl = w % 2

    def seq_of(dz, dy):
        return ((zh + dz) % 4) * 8 + ((y + dy) % 4) * 2 + core

    def wgt_of(dx, dz):
        return ((x + dx) % 4) * 2 + (zl + dz) % 2

    sibling = s + 1 - 2 * core

    def on_seq(i):
        return {"seq": i, "wgt": w}

    def on_wgt(i):
        return {"seq": s, "wgt": i}

    def copy(src, dst, send_sem, recv_sem, device):
        return pltpu.make_async_remote_copy(
            src_ref=src,
            dst_ref=dst,
            send_sem=send_sem,
            recv_sem=recv_sem,
            device_id=device,
            device_id_type=MESH,
        )

    here = on_seq(sibling)

    def arrived(dst, sem):
        copy(dst, dst, send.at[0, 0], sem, here).wait_recv()

    def sent(region, sem):
        copy(region, region, sem, w_recv.at[0, 0, 0, 0], here).wait_send()

    def w_slot(l, half, index):
        if half == 0:
            return WA.at[l, index]
        if half == 1:
            return WB.at[l, index]
        return O.at[l, 2 * index + (half - 2)]

    def w_sem(l, half, dz, dy):
        if half < 2:
            return w_recv.at[l, half, dz, dy]
        return o_recv.at[l, half - 2, dz, dy]

    def w_to(l, half, owner, rel, step):
        slot = w_slot(l, half, owner)
        to = ((rel[0] - step[0]) % 4, (rel[1] - step[1]) % 4)
        copy(
            slot, slot, send.at[l, half], w_sem(l, half, *to), on_seq(seq_of(*step))
        ).start()

    def w_to_sibling(l, half, owner):
        slot = w_slot(l, half, owner)
        copy(slot, slot, send.at[l, half], sib_recv.at[l, half], here).start()

    def w_own(l, halves, along="yz"):
        for half in halves:
            if "y" in along:
                w_to(l, half, s, (0, 0), (0, 1))
                w_to(l, half, s, (0, 0), (0, 3))
                w_to_sibling(l, half, s)
            if "z" in along:
                w_to(l, half, s, (0, 0), (1, 0))
                w_to(l, half, s, (0, 0), (3, 0))

    def w_event(l, half, dz, dy):
        owner = seq_of(dz, dy)
        arrived(w_slot(l, half, owner), w_sem(l, half, dz, dy))
        for step in w_forwards(half, dz, dy):
            w_to(l, half, owner, (dz, dy), step)
        w_to_sibling(l, half, owner)

    def h_to(l, piece, rel, step):
        slot = H.at[l, 4 * wgt_of(*rel) + piece]
        to = ((rel[0] - step[0]) % 4, (rel[1] - step[1]) % 2)
        copy(
            slot, slot, send.at[l, 4], h_recv.at[l, to[0], to[1], piece], on_wgt(wgt_of(*step))
        ).start()

    def m_to(l, piece, rel, step):
        slot = MX.at[l, wgt_of(*rel), piece]
        to = ((rel[0] - step[0]) % 4, (rel[1] - step[1]) % 2)
        copy(
            slot, slot, send.at[l, 5], mx_recv.at[l, to[0], to[1], piece], on_wgt(wgt_of(*step))
        ).start()

    def h_event(l, piece, dx, dz):
        arrived(H.at[l, 4 * wgt_of(dx, dz) + piece], h_recv.at[l, dx, dz, piece])
        for step in a_forwards(BY_Z["h"][l], piece, dx, dz):
            h_to(l, piece, (dx, dz), step)

    def m_event(l, piece, dx, dz):
        arrived(MX.at[l, wgt_of(dx, dz), piece], mx_recv.at[l, dx, dz, piece])
        for step in a_forwards(BY_Z["m"][l], piece, dx, dz):
            m_to(l, piece, (dx, dz), step)

    peers = [(dx, dz) for dz in range(2) for dx in range(4) if (dx, dz) != (0, 0)]

    def share_squares(l, kind, row):
        SS[l, kind, w] = row
        slot = SS.at[l, kind, w]
        for rel in peers:
            copy(
                slot, slot, send.at[l, 6 + kind], ss_recv.at[l, kind], on_wgt(wgt_of(*rel))
            ).start()

    def all_squares(l, kind):
        arrived(SS.at[l, kind, pl.ds(0, 7)], ss_recv.at[l, kind])
        return jnp.sum(SS[l, kind], axis=0)

    def gain(l, kind, rows):
        return gains[rows, 2 * kind + l : 2 * kind + l + 1]

    def dequantize(l):
        for j, (dst, src) in enumerate(
            (
                (WA.at[l, s, :, 0:128], wq.at[l, :, 0:128]),
                (WA.at[l, s, :, 128:256], wq.at[l, :, 128:256]),
                (WB.at[l, s, :, 0:128], wk.at[l]),
                (WB.at[l, s, :, 128:256], wv.at[l]),
            )
        ):
            dst[...] = src[...] * factors[l, :, j : j + 1]
        for half in range(2):
            O[l, 2 * s + half] = wo[l, 32 * half : 32 * half + 32] * o_factors[l : l + 1]

    dequantize(0)
    for l in range(LAYERS):
        for slot in range(3):
            KV[l, slot] = jnp.zeros((2, HD, TOK), BF)

    barrier = pltpu.get_barrier_semaphore()
    neighbours = [here]
    neighbours += [on_seq(seq_of(*step)) for step in ((0, 1), (0, 3), (1, 0), (3, 0))]
    neighbours += [on_wgt(wgt_of(*rel)) for rel in peers]
    after = on_seq((s + 2) % NSEQ)
    neighbours += [after, on_seq((s + NSEQ - 2) % NSEQ)]
    neighbours += [on_seq((s + NSEQ - 3 + 6 * core) % NSEQ)]
    for device in neighbours:
        pl.semaphore_signal(barrier, inc=1, device_id=device, device_id_type=MESH)
    pl.semaphore_wait(barrier, len(neighbours))

    late = pl.ds(128, 256)

    def scale(l):
        row = lax.rsqrt(all_squares(l - 1, 1) / D + eps) if l else None
        squares = jnp.zeros((1, TOK), F32)
        for i in (0, 3, 1, 2):
            if l == 0:
                out[i] = hid[i]
                state = hid[i].astype(F32)
            else:
                out[i] = next_state(l - 1, i, row)
                state = out[i].astype(F32)
            H[l, 4 * w + i] = (state * gain(l, 0, pl.ds(ROWS * i, ROWS))).astype(BF)
            squares += jnp.sum(state * state, axis=0, keepdims=True)
            h_to(l, i, (0, 0), (1, 0) if i < 2 else (3, 0))
        for i in (2, 3):
            h_to(l, i, (0, 0), (1, 0))
            h_to(l, 3 - i, (0, 0), (3, 0))
        share_squares(l, 0, squares)
        acc[...] = jnp.zeros_like(acc)
    def multiply(l, half, first, last):
        buf, rows = ((WA, pl.ds(0, 256)), (WB, pl.ds(256, 256)))[half]

        def one(group, carry):
            k = group % 4
            index = 4 * wgt_of(k * (k + 1) // 2, group // 4)
            total = acc[rows]
            for i in range(4):
                total += contract_rows(buf[l, index + i], H[l, index + i])
            acc[rows] = total
            return carry

        lax.fori_loop(first, last, one, 0)

    def head_of(l, rows, row, kind):
        values = acc[rows] * row
        values *= lax.rsqrt(jnp.mean(values * values, axis=0, keepdims=True) + eps)
        values *= gain(l, kind, pl.ds(WIDTH, HD))
        first = values[0:64]
        second = values[64:128]
        c = cosine[...]
        n = sine[...]
        return first * c - second * n, second * c + first * n

    def kv_sibling(l, slot, part):
        copy(
            KV.at[l, slot, part], KV.at[l, 2, part],
            send.at[l, 9], kv_recv.at[l, 2, part], here,
        ).start()

    def kv_far(l, slot, part, device):
        copy(
            KV.at[l, slot, part, :, late], KV.at[l, 0, part, :, late],
            send.at[l, 10], kv_recv.at[l, 0, part], device,
        ).start()

    def kv_next(l, part, rows):
        copy(
            KV.at[l, 3, part, rows], KV.at[l, 1, part, rows],
            send.at[l, 8], kv_recv.at[l, 1, part], after,
        ).start()

    corner = [pl.ds(64 + 32 * i, 32) for i in range(2)]

    def keys_values(l):
        row = lax.rsqrt(all_squares(l, 0) / D + eps)
        ROW[...] = row
        KV[l, 3, 1] = (acc[384:512] * row).astype(BF)

        @pl.when((y == 3) & (s < NSEQ - 2))
        def _():
            for i in range(2):
                copy(
                    KV.at[l, 3, 1, corner[i]], RB.at[l, pl.ds(32 * i, 32)],
                    send.at[l, 8], kv_recv.at[l, 3, i], on_seq(s - 6),
                ).start()

        first, second = head_of(l, pl.ds(256, 128), row, 1)
        KV[l, 3, 0, 0:64] = first.astype(BF)
        KV[l, 3, 0, 64:128] = second.astype(BF)

        @pl.when(s < NSEQ - 2)
        def _():
            kv_next(l, 0, pl.ds(0, 128))
            kv_next(l, 1, pl.ds(0, 64))

        @pl.when((y != 3) & (s < NSEQ - 2))
        def _():
            kv_next(l, 1, pl.ds(64, 64))

        @pl.when(core == 0)
        def _():
            for part in range(2):
                kv_sibling(l, 3, part)

        @pl.when((core == 1) & (s < NSEQ - 3))
        def _():
            for part in range(2):
                kv_far(l, 3, part, on_seq((s + 3) % NSEQ))

    def queries(l):
        for h in range(2):
            first, second = head_of(l, pl.ds(128 * h, 128), ROW[...], 0)
            Q[h, 0:64] = (first * query_scale).astype(BF)
            Q[h, 64:128] = (second * query_scale).astype(BF)

    def attend(l, slot):
        skip = 128 if slot == 0 else 0
        rows = TOK - skip
        window = windows[l]
        KX[0:rows] = KV[l, slot, 0, :, skip:TOK].T
        keys = lax.broadcasted_iota(jnp.int32, (rows, 128), 0) + (TOK * slot + skip)
        for h in range(2):
            SC[h, 0:rows] = jnp.dot(KX[0:rows], Q[h], preferred_element_type=F32)
        for h in range(2):
            for c in range(3):
                lanes = pl.ds(128 * c, 128)
                gap = lax.broadcasted_iota(jnp.int32, (rows, 128), 1) + (128 * c + 3 * TOK) - keys
                allowed = (gap < window) & (keys >= 3 * TOK - TOK * s)
                if slot == 3:
                    allowed &= gap >= 0
                weight = jnp.where(allowed, jnp.exp(SC[h, 0:rows, lanes]), 0.0)
                total = jnp.sum(weight, axis=0, keepdims=True)
                if slot != 3:
                    total += TOT[h, :, lanes]
                TOT[h, :, lanes] = total
                PB[h, 0:rows, lanes] = weight.astype(BF)
            mixed = jnp.dot(
                KV[l, slot, 1, :, skip:TOK], PB[h, 0:rows], preferred_element_type=F32
            )
            if slot != 3:
                mixed += MIX[h]
            MIX[h] = mixed
        if slot == 0:
            for h in range(2):
                mixed = (MIX[h] * (1.0 / TOT[h])).astype(BF)
                MX[l, w, 2 * h] = mixed[0:64]
                MX[l, w, 2 * h + 1] = mixed[64:128]
            for i in range(4):
                for piece, step in ((i, (1, 0)), (3 - i, (3, 0)), ((0, 3, 1, 2)[i], (0, 1))):
                    m_to(l, piece, (0, 0), step)
            proj[...] = jnp.zeros_like(proj)

    def kv_event(l, slot):
        if slot == 1:

            @pl.when((y == 0) & (s < NSEQ - 8))
            def _():
                for i in range(2):
                    rows = RB.at[l, pl.ds(32 * i, 32)]
                    arrived(rows, kv_recv.at[l, 3, i])
                    copy(
                        rows, KV.at[l, 1, 1, corner[i]],
                        send.at[l, 11], kv_recv.at[l, 1, 1], on_seq(s + 8),
                    ).start()

            for part in range(2):

                @pl.when(s >= 2)
                def _():
                    arrived(KV.at[l, 1, part], kv_recv.at[l, 1, part])

                @pl.when((core == 0) & (s >= 2))
                def _():
                    kv_far(l, 1, part, here)

                @pl.when((core == 1) & (s >= 2))
                def _():
                    kv_sibling(l, 1, part)

        if slot == 2:

            @pl.when(s >= 1)
            def _():
                for part in range(2):
                    arrived(KV.at[l, 2, part], kv_recv.at[l, 2, part])

        if slot == 0:

            @pl.when(s >= 3)
            def _():
                for part in range(2):
                    arrived(KV.at[l, 0, part, :, late], kv_recv.at[l, 0, part])

    def project(l, first, last):
        def one(group, carry):
            k = group % 4
            index = wgt_of(k * (k + 1) // 2, group // 4)
            block = O[l, pl.ds(8 * index, 8)].reshape(256, WIDTH)
            proj[...] += contract_rows(block, MX[l, index].reshape(256, TOK))
            return carry

        lax.fori_loop(first, last, one, 0)

    def share(l):
        squares = jnp.zeros((1, TOK), F32)
        for i in range(4):
            part = proj[ROWS * i : ROWS * (i + 1)]
            squares += jnp.sum(part * part, axis=0, keepdims=True)
        share_squares(l, 1, squares)

    def next_state(l, i, row):
        rows = pl.ds(ROWS * i, ROWS)
        post = proj[rows] * row * gain(l, 1, rows)
        return (out[i].astype(F32) + post).astype(BF)

    def finish(l):
        if l == LAYERS - 1:
            row = lax.rsqrt(all_squares(l, 1) / D + eps)
            for i in range(4):
                out[i] = next_state(l, i, row)

    steps = []
    for name in schedule():
        if name[0] in ("mm", "pj"):
            *key, group = name
            if steps and steps[-1][:-2] == tuple(key) and steps[-1][-1] == group:
                steps[-1] = (*steps[-1][:-1], group + 1)
            else:
                steps.append((*key, group, group + 1))
        else:
            steps.append(name)

    for kind, l, *which in steps:
        if kind == "w":
            w_event(l, *which)
        elif kind == "h":
            h_event(l, *which)
        elif kind == "m":
            m_event(l, *which)
        elif kind == "mm":
            multiply(l, *which)
        elif kind == "pj":
            project(l, *which)
        elif kind == "scale":
            scale(l)
        elif kind == "wown":
            w_own(l, (1, 0))
        elif kind == "oown":
            w_own(l, (2, 3))
        elif kind == "hz":
            for i in (0, 3, 1, 2):
                h_to(l, i, (0, 0), (0, 1))
            if l == 0:
                dequantize(1)
        elif kind == "wsib":
            half = which[0]
            arrived((WA, WB)[half].at[l, pl.ds(0, 16)], sib_recv.at[l, half])
        elif kind == "osib":
            for half in (2, 3):
                arrived(O.at[l, pl.ds(0, 16)], sib_recv.at[l, half])
        elif kind == "kvsent":
            keys_values(l)
        elif kind == "heads":
            queries(l)
        elif kind in ("kv0", "kv1", "kv2"):
            kv_event(l, int(kind[2]))
        elif kind in ("att0", "att1", "att2", "att3"):
            attend(l, int(kind[3]))
        elif kind == "share":
            share(l)
        elif kind == "fin":
            finish(l)

    for l in range(LAYERS):
        sent(WA.at[l, pl.ds(0, 31)], send.at[l, 0])
        sent(WB.at[l, pl.ds(0, 31)], send.at[l, 1])
        sent(O.at[l, pl.ds(0, 31)], send.at[l, 2])
        sent(O.at[l, pl.ds(0, 31)], send.at[l, 3])
        sent(H.at[l, pl.ds(0, 28)], send.at[l, 4])
        sent(MX.at[l, pl.ds(0, 7)], send.at[l, 5])
        for kind in range(2):
            sent(SS.at[l, kind, pl.ds(0, 7)], send.at[l, 6 + kind])

        @pl.when(s < NSEQ - 2)
        def _():
            sent(KV.at[l, 1], send.at[l, 8])

        @pl.when((y == 0) & (s < NSEQ - 8))
        def _():
            sent(RB.at[l], send.at[l, 11])

        @pl.when((core == 0) | (s >= 2))
        def _():
            sent(KV.at[l, 2], send.at[l, 9])

        @pl.when(((core == 0) & (s >= 2)) | ((core == 1) & (s < NSEQ - 3)))
        def _():
            sent(KV.at[l, 0, :, :, late], send.at[l, 10])


def row_factors(scale_codes, first_row, rows):
    blocks = (first_row + jnp.arange(rows, dtype=jnp.int32)) // BLOCK
    pick = blocks[:, None] == jnp.arange(scale_codes.shape[1], dtype=jnp.int32)[None, :]
    factor = jnp.exp2(scale_codes.astype(F32) - 127.0)
    return jnp.sum(jnp.where(pick[None, :, :, None], factor[:, None], 0.0), axis=2)


def per_device(
    hidden,
    q_weight,
    k_weight,
    v_weight,
    o_weight,
    q_scale,
    k_scale,
    v_scale,
    o_scale,
    in_gain,
    post_gain,
    q_gain,
    k_gain,
    windows,
):
    s = lax.axis_index("seq")
    w = lax.axis_index("wgt")
    scales = jnp.concatenate([q_scale, k_scale, v_scale], axis=2)
    factors = row_factors(scales, ROWS * s, ROWS).astype(BF)
    o_rows = jnp.exp2(
        lax.dynamic_slice_in_dim(o_scale, s // 2, 1, axis=1).astype(F32) - 127.0
    )
    columns = (w * WIDTH + jnp.arange(WIDTH, dtype=jnp.int32)) // BLOCK
    pick = columns[:, None] == jnp.arange(D // BLOCK, dtype=jnp.int32)[None, :]
    o_factor = jnp.sum(jnp.where(pick[None], o_rows, 0.0), axis=2).astype(BF)
    gin = lax.dynamic_slice_in_dim(in_gain, w * WIDTH, WIDTH, axis=1)
    gains = jnp.concatenate(
        [
            jnp.concatenate([gin, post_gain, jnp.zeros((4, WIDTH), F32)], axis=0),
            jnp.concatenate([q_gain, k_gain, jnp.zeros((4, HD), F32)], axis=0),
        ],
        axis=1,
    ).T
    half = HD // 2
    position = s * TOK + jnp.arange(TOK, dtype=jnp.int32)
    inverse = rope_base ** (-jnp.arange(half, dtype=F32) * 2.0 / HD)
    angles = inverse[:, None] * position.astype(F32)[None, :]
    hid = hidden.T.reshape(4, ROWS, TOK)

    vmem = pl.BlockSpec(memory_space=pltpu.VMEM)
    dma = pltpu.SemaphoreType.DMA
    state = pl.pallas_call(
        kernel,
        out_shape=jax.ShapeDtypeStruct((4, ROWS, TOK), BF),
        in_specs=[vmem] * 10 + [pl.BlockSpec(memory_space=pltpu.SMEM)],
        out_specs=vmem,
        scratch_shapes=[
            pltpu.VMEM((LAYERS, 32, ROWS, TOK), BF),
            pltpu.VMEM((LAYERS, NSEQ, ROWS, 256), BF),
            pltpu.VMEM((LAYERS, NSEQ, ROWS, 256), BF),
            pltpu.VMEM((LAYERS, 2 * NSEQ, 32, WIDTH), BF),
            pltpu.VMEM((LAYERS, NWGT, 4, HD // 2, TOK), BF),
            pltpu.VMEM((LAYERS, 4, 2, HD, TOK), BF),
            pltpu.VMEM((LAYERS, 2, NWGT, 1, TOK), F32),
            pltpu.VMEM((512, TOK), F32),
            pltpu.VMEM((2, HD, TOK), BF),
            pltpu.VMEM((1, TOK), F32),
            pltpu.VMEM((TOK, HD), BF),
            pltpu.VMEM((2, TOK, TOK), F32),
            pltpu.VMEM((2, TOK, TOK), BF),
            pltpu.VMEM((2, 1, TOK), F32),
            pltpu.VMEM((2, HD, TOK), F32),
            pltpu.VMEM((LAYERS, HD // 2, TOK), BF),
            pltpu.VMEM((WIDTH, TOK), F32),
            dma((LAYERS, 2, 4, 4)),
            dma((LAYERS, 2, 4, 4)),
            dma((LAYERS, 4, 2, 4)),
            dma((LAYERS, 4, 2, 4)),
            dma((LAYERS, 4, 2)),
            dma((LAYERS, 4)),
            dma((LAYERS, 2)),
            dma((LAYERS, 12)),
        ],
        compiler_params=pltpu.CompilerParams(
            collective_id=0, has_side_effects=True, vmem_limit_bytes=44 * 1024 * 1024
        ),
    )(
        hid,
        q_weight,
        k_weight,
        v_weight,
        o_weight,
        factors,
        o_factor,
        gains,
        jnp.cos(angles),
        jnp.sin(angles),
        windows,
    )
    return state.reshape(WIDTH, TOK).T


def solution(mesh):
    in_specs = (
        P("seq", "wgt"),
        P(None, "seq", "wgt"),
        P(None, "seq", "wgt"),
        P(None, "seq", "wgt"),
        P(None, "seq", "wgt"),
        P(None, None, "wgt"),
        P(None, None, "wgt"),
        P(None, None, "wgt"),
        P(),
        P(),
        P(None, "wgt"),
        P(),
        P(),
        P(),
    )
    return jax.shard_map(
        per_device, mesh=mesh, in_specs=in_specs, out_specs=P("seq", "wgt"), check_vma=False
    )
```
